128 devices in a mesh: heads: 1, cp: 128 (over z, y, x, core).
Axes of the slice: x: 4, y: 4, z: 4, core: 2. Of those that a mesh axis runs over, the one named last changes fastest.
Arguments:
- query: bfloat16 [2, 2048, 32, 128], P(None, 'cp', 'heads')
- attn_out: bfloat16 [2, 2048, 32, 128], P(None, 'cp', 'heads')
- grad_out: bfloat16 [2, 2048, 32, 128], P(None, 'cp', 'heads')
- row_lse: float32 [2, 2048, 32], P(None, 'cp', 'heads')
- key_cache: bfloat16 [12288, 8, 128], P('cp', 'heads')
- value_cache: bfloat16 [12288, 8, 128], P('cp', 'heads')
Outputs:
- output 1: bfloat16 [2, 2048, 32, 128], P(None, 'cp', 'heads')
- output 2: float32 [12288, 8, 128], P('cp', 'heads')
- output 3: float32 [12288, 8, 128], P('cp', 'heads')
All inputs are finite; a program needn't handle non-finite values.
Results may differ from the reference program's by a relative error of at most 0.00468.
Values are sent between devices in bfloat16 or wider.
A program may use at most 1 GiB of HBM per device.

```python
import jax
import jax.numpy as jnp
from jax import lax

NUM_SLICES = 2
SLICE_LEN = 2048
PREFIX0 = 8192
Q_HEADS = 32
KV_HEADS = 8
HEAD_DIM = 128

GROUP = Q_HEADS // KV_HEADS
ROW_BLOCK = max(1, 128 // Q_HEADS)
NUM_BLOCKS = SLICE_LEN // ROW_BLOCK
PREFIX_LEN = PREFIX0 + NUM_SLICES * SLICE_LEN


def forward_lse(query, key_cache):
    inv_sqrt = HEAD_DIM ** -0.5
    k_full = key_cache.astype(jnp.float32)
    lse_list = []
    for slice_idx in range(NUM_SLICES):
        key_end = PREFIX0 + (slice_idx + 1) * SLICE_LEN
        base_pos = PREFIX0 + slice_idx * SLICE_LEN
        k_part = k_full[:key_end]
        key_pos = jnp.arange(key_end)
        q_blocks = query[slice_idx].astype(jnp.float32).reshape(NUM_BLOCKS, ROW_BLOCK, KV_HEADS, GROUP, HEAD_DIM)

        def block_lse(scan_in):
            q_blk, blk_idx = scan_in
            query_pos = base_pos + blk_idx * ROW_BLOCK + jnp.arange(ROW_BLOCK)
            visible = (key_pos[None, :] <= query_pos[:, None])[:, None, None, :]
            scores = jnp.einsum('rhgd,khd->rhgk', q_blk, k_part) * inv_sqrt
            scores = jnp.where(visible, scores, -1e30)
            return jax.nn.logsumexp(scores, axis=-1)

        lse_blocks = lax.map(block_lse, (q_blocks, jnp.arange(NUM_BLOCKS)))
        lse_list.append(lse_blocks.reshape(SLICE_LEN, Q_HEADS))
    return jnp.stack(lse_list)


def setup_inputs(seed: int = 0, part: int = 0) -> dict:
    base_key = jax.random.fold_in(jax.random.key(seed), part)
    key_list = jax.random.split(base_key, 6)
    q_shape = (NUM_SLICES, SLICE_LEN, Q_HEADS, HEAD_DIM)
    kv_shape = (PREFIX_LEN, KV_HEADS, HEAD_DIM)
    token_scale = jax.random.uniform(key_list[0], (NUM_SLICES, SLICE_LEN, Q_HEADS, 1), jnp.float32, minval=0.5, maxval=1.6)
    query = (jax.random.normal(key_list[1], q_shape, jnp.float32) * token_scale).astype(jnp.bfloat16)
    key_cache = jax.random.normal(key_list[2], kv_shape, jnp.float32).astype(jnp.bfloat16)
    value_cache = jax.random.normal(key_list[3], kv_shape, jnp.float32).astype(jnp.bfloat16)
    grad_f = 3.0 * jax.random.normal(key_list[4], q_shape, jnp.float32)
    out_f = 0.07 * grad_f + 0.6 * jax.random.normal(key_list[5], q_shape, jnp.float32)
    row_lse = forward_lse(query, key_cache).astype(jnp.float32)
    return {'query': query, 'attn_out': out_f.astype(jnp.bfloat16), 'grad_out': grad_f.astype(jnp.bfloat16), 'row_lse': row_lse, 'key_cache': key_cache, 'value_cache': value_cache}


def reference(query, attn_out, grad_out, row_lse, key_cache, value_cache):
    inv_sqrt = HEAD_DIM ** -0.5
    k_full = key_cache.astype(jnp.float32)
    v_full = value_cache.astype(jnp.float32)
    grad_k = jnp.zeros((PREFIX_LEN, KV_HEADS, HEAD_DIM), jnp.float32)
    grad_v = jnp.zeros((PREFIX_LEN, KV_HEADS, HEAD_DIM), jnp.float32)
    blk_shape = (NUM_BLOCKS, ROW_BLOCK, KV_HEADS, GROUP, HEAD_DIM)
    dq_list = []
    for slice_idx in range(NUM_SLICES):
        key_end = PREFIX0 + (slice_idx + 1) * SLICE_LEN
        base_pos = PREFIX0 + slice_idx * SLICE_LEN
        k_part = k_full[:key_end]
        v_part = v_full[:key_end]
        key_pos = jnp.arange(key_end)
        q_blocks = query[slice_idx].astype(jnp.float32).reshape(blk_shape)
        o_blocks = attn_out[slice_idx].astype(jnp.float32).reshape(blk_shape)
        do_blocks = grad_out[slice_idx].astype(jnp.float32).reshape(blk_shape)
        lse_blocks = row_lse[slice_idx].reshape(NUM_BLOCKS, ROW_BLOCK, KV_HEADS, GROUP)

        def block_step(acc_pair, scan_in):
            dk_acc, dv_acc = acc_pair
            q_blk, o_blk, do_blk, lse_blk, blk_idx = scan_in
            query_pos = base_pos + blk_idx * ROW_BLOCK + jnp.arange(ROW_BLOCK)
            visible = (key_pos[None, :] <= query_pos[:, None])[:, None, None, :]
            row_delta = jnp.sum(do_blk * o_blk, axis=-1)
            scores = jnp.einsum('rhgd,khd->rhgk', q_blk, k_part) * inv_sqrt
            prob_mat = jnp.where(visible, jnp.exp(scores - lse_blk[..., None]), 0.0)
            prob_bf = prob_mat.astype(jnp.bfloat16).astype(jnp.float32)
            dv_acc = dv_acc + jnp.einsum('rhgk,rhgd->khd', prob_bf, do_blk)
            d_prob = jnp.einsum('rhgd,khd->rhgk', do_blk, v_part)
            d_scores = (prob_mat * (d_prob - row_delta[..., None])).astype(jnp.bfloat16).astype(jnp.float32)
            dq_blk = jnp.einsum('rhgk,khd->rhgd', d_scores, k_part) * inv_sqrt
            dk_acc = dk_acc + jnp.einsum('rhgk,rhgd->khd', d_scores, q_blk) * inv_sqrt
            return (dk_acc, dv_acc), dq_blk.astype(jnp.bfloat16)

        init_pair = (grad_k[:key_end], grad_v[:key_end])
        scan_xs = (q_blocks, o_blocks, do_blocks, lse_blocks, jnp.arange(NUM_BLOCKS))
        (dk_part, dv_part), dq_blocks = lax.scan(block_step, init_pair, scan_xs)
        grad_k = jnp.concatenate([dk_part, grad_k[key_end:]], axis=0)
        grad_v = jnp.concatenate([dv_part, grad_v[key_end:]], axis=0)
        dq_list.append(dq_blocks.reshape(SLICE_LEN, Q_HEADS, HEAD_DIM))
    return (jnp.stack(dq_list), grad_k, grad_v)
```

```python
import functools

import jax
import jax.numpy as jnp
from jax import lax
from jax.experimental import pallas as pl
from jax.experimental.pallas import tpu as pltpu
from jax.sharding import PartitionSpec as P

F32 = jnp.float32
BF16 = jnp.bfloat16
MESH = pl.DeviceIdType.MESH
LOG2E = 1.4426950408889634


class Lazy:
    def __init__(self, makers):
        self.makers = makers

    def __getitem__(self, i):
        return Lazy(self.makers[i]) if isinstance(i, slice) else self.makers[i]()

    def __add__(self, other):
        return Lazy(self.makers + other.makers)

    def __iter__(self):
        return (m() for m in self.makers)


def kernel(shape, msg, ld, dq_out, dkv_out, qd, kv, ldg, qt, kt, lb, db, dq,
           acc, part, rak, rbk, raq, rbq, outk, outq,
           a_send, a_q, a_kv, a_ld, f_send, x_rp, x_rm, x_hp, x_hm, l_r,
           y_rp, y_rm, y_hp, y_hm, k_send, ka, kb, kd, q_send, qa, qb, qd_s,
           o_send, ok_r, oq_r):
    n_slices, rows_dev, kv_heads, group, head_dim, keys_dev, cp_size = shape
    slice_len = rows_dev * cp_size
    prefix0 = keys_dev * cp_size - n_slices * slice_len
    inv_sqrt = head_dim ** -0.5
    c2 = inv_sqrt * LOG2E
    me = lax.axis_index("cp")
    core = lax.rem(me, 2)
    xi = lax.rem(me // 2, 4)
    yi = lax.rem(me // 8, 4)
    zi = me // 32

    def dev(z, y, x, c):
        return {"cp": z * 32 + y * 8 + x * 2 + c}

    def ring(i, d):
        return lax.rem(i + d + 4, 4)

    xp, xm = dev(zi, yi, ring(xi, 1), core), dev(zi, yi, ring(xi, -1), core)
    yp, ym = dev(zi, ring(yi, 1), xi, core), dev(zi, ring(yi, -1), xi, core)
    x2 = dev(zi, yi, ring(xi, 2), core)
    offs = (0, 1, 3, 2)

    def off_in(s):
        return s ^ (s >> 1)

    def off_out(s):
        return off_in(3 - s)

    def rcopy(src, dst, ss, rs, to):
        return pltpu.make_async_remote_copy(src_ref=src, dst_ref=dst, send_sem=ss, recv_sem=rs,
                                            device_id=to, device_id_type=MESH)

    barrier = pltpu.get_barrier_semaphore()
    peers = [xp, xm, x2, yp, ym]
    for o in offs:
        for dc in range(2):
            if o or dc:
                peers.append(dev(ring(zi, o), yi, xi, core ^ dc))
    for p in peers:
        pl.semaphore_signal(barrier, inc=1, device_id=p, device_id_type=MESH)
    pl.semaphore_wait(barrier, len(peers))

    def a2a(o, dc):
        tz, tc = ring(zi, o), core ^ dc
        head = tz * 2 + tc
        to = dev(tz, yi, xi, tc)
        k = o * 2 + dc
        return Lazy([
            lambda: rcopy(msg.at[head, pl.ds(0, 256)].reshape(2, 2, 64, 128), qd.at[zi, :, :, xi, core], a_send.at[k, 0], a_q.at[k], to),
            lambda: rcopy(msg.at[head, pl.ds(256, 192)].reshape(2, 96, 128), kv.at[zi, :, yi, core], a_send.at[k, 1], a_kv.at[k], to),
            lambda: rcopy(ld.at[head], ldg.at[zi, xi, core], a_send.at[k, 2], a_ld.at[k], to),
        ])

    for o in offs:
        for dc in (1, 0):
            if o or dc:
                for c in a2a(o, dc):
                    c.start()
    head = zi * 2 + core
    qd[zi, :, :, xi, core] = msg[head, 0:256].reshape(2, 2, 64, 128)
    kv[zi, :, yi, core] = msg[head, 256:448].reshape(2, 96, 128)
    ldg[zi, xi, core] = ld[head]

    def forward(o):
        sz = ring(zi, -o)
        for dc in (1, 0):
            if o or dc:
                for c in a2a(o, dc):
                    c.wait_recv()
        k = o
        for c in fcopies(sz, k):
            c.start()

    def fcopies(sz, k):
        qc = qd.at[sz, :, :, xi]
        kc = kv.at[sz, :, yi]
        lc = ldg.at[sz, xi]
        return Lazy([lambda: rcopy(qc, qc, f_send.at[k, 0], x_rp.at[k], xp), lambda: rcopy(qc, qc, f_send.at[k, 1], x_rm.at[k], xm),
                lambda: rcopy(kc, kc, f_send.at[k, 2], y_rp.at[k], yp), lambda: rcopy(kc, kc, f_send.at[k, 3], y_rm.at[k], ym),
                lambda: rcopy(lc, lc, f_send.at[k, 4], l_r.at[k, 0], xp), lambda: rcopy(lc, lc, f_send.at[k, 5], l_r.at[k, 1], xm),
                lambda: rcopy(lc, lc, f_send.at[k, 6], l_r.at[k, 2], x2)])

    def rcopies(sz, k):
        qm = qd.at[sz, 0, :, ring(xi, -1)]
        qp = qd.at[sz, 1, :, ring(xi, 1)]
        km = kv.at[sz, 0, ring(yi, -1)]
        kp = kv.at[sz, 1, ring(yi, 1)]
        return Lazy([lambda: rcopy(qm, qm, f_send.at[k, 7], x_hp.at[k], xp), lambda: rcopy(qp, qp, f_send.at[k, 8], x_hm.at[k], xm),
                lambda: rcopy(km, km, f_send.at[k, 9], y_hp.at[k], yp), lambda: rcopy(kp, kp, f_send.at[k, 10], y_hm.at[k], ym)])

    def relay(o):
        sz = ring(zi, -o)
        f = fcopies(sz, o)
        r = rcopies(sz, o)
        f[0].wait_recv()
        r[0].start()
        f[1].wait_recv()
        r[1].start()
        f[2].wait_recv()
        r[2].start()
        f[3].wait_recv()
        r[3].start()

    def arrive(o):
        sz = ring(zi, -o)
        for c in rcopies(sz, o):
            c.wait_recv()
        for c in fcopies(sz, o)[4:]:
            c.wait_recv()

    def prep(o):
        sz = ring(zi, -o)
        for a in range(2):
            qt[sz, a] = qd[sz, a].reshape(1024, 128).T
            kt[sz, a] = kv[sz, a].reshape(768, 128).T
        for x in range(4):
            for c in range(2):
                for ref, r in ((lb, 0), (db, 1)):
                    t = jnp.broadcast_to(ldg[sz, x, c, r:r + 1, :], (128, 128)).T
                    ref[sz, 0, x, pl.ds(c * 64, 64)] = t[:64]
                    ref[sz, 1, x, pl.ds(c * 64, 64)] = t[64:]

    for i in range(4):
        forward(offs[i])
        if i:
            relay(offs[i - 1])
    relay(offs[3])
    for i in range(4):
        arrive(offs[i])
        prep(offs[i])

    dq[...] = jnp.zeros_like(dq)

    def tile(zq, zk, j, k0, nk, masked):
        if j is None:
            rows, rsl, jsl = 1024, slice(None), slice(None)
        else:
            rows, rsl, jsl = 512, pl.ds(pl.multiple_of(j * 512, 512), 512), j
        ks = pl.ds(k0, nk)
        q = qd[zq, 0, jsl].reshape(rows, 128)
        do = qd[zq, 1, jsl].reshape(rows, 128)
        lrow = lb[zq, jsl].reshape(rows, 128)
        drow = db[zq, jsl].reshape(rows, 128)
        kn = kv[zk, 0].reshape(768, 128)[k0:k0 + nk] if isinstance(k0, int) else kv[zk, 0].reshape(768, 128)
        s = jnp.dot(q, kt[zk, 0, :, ks], preferred_element_type=F32)
        p = jnp.exp2(s * c2 - jnp.concatenate([lrow] * (nk // 128), 1))
        if masked:
            kid = lax.broadcasted_iota(jnp.int32, (1, nk), 1) + k0
            run = (kid >= 192).astype(jnp.int32) + (kid >= 384).astype(jnp.int32) + (kid >= 576).astype(jnp.int32)
            kpos = zk * 3072 + xi * 192 + kid + run * 576
            qbase = prefix0 + j * slice_len + zq * 512 + yi * 128
            qrow = lax.broadcasted_iota(jnp.int32, (rows, nk), 0) >> 2
            p = jnp.where(kpos - qbase <= qrow, p, 0.0)
        pb = p.astype(BF16)
        dp = jnp.dot(do, kt[zk, 1, :, ks], preferred_element_type=F32)
        ds = (p * (dp - jnp.concatenate([drow] * (nk // 128), 1))).astype(BF16)
        acc[1, :, ks] += jnp.dot(qt[zq, 1, :, rsl], pb, preferred_element_type=F32)
        acc[0, :, ks] += jnp.dot(qt[zq, 0, :, rsl], ds, preferred_element_type=F32)
        r = jnp.dot(ds, kn, preferred_element_type=F32)
        dq[zq, jsl] += r.reshape((2, 4, 128, 128) if j is None else (4, 128, 128))

    def cell(zq, zk):
        @pl.when(zk <= 1)
        def _():
            tile(zq, zk, None, 0, 768, False)

        @pl.when(zk == 2)
        def _():
            tile(zq, zk, 1, 0, 768, False)

        @pl.when(zk >= 2)
        def _():
            tile(zq, zk, zk - 2, 0, 768, True)

        @pl.when(zk == 3)
        def _():
            last = prefix0 + zq * 512 + yi * 128 + 127
            first = 3 * 3072 + xi * 192

            @pl.when(first <= last)
            def _():
                tile(zq, zk, 0, 0, 256, True)

            @pl.when(first + 768 + 64 <= last)
            def _():
                tile(zq, zk, 0, 256, 256, True)

    h0, h1 = pl.ds(0, 96), pl.ds(96, 96)
    yP, yM, yO = ring(yi, 1), ring(yi, -1), ring(yi, 2)
    xP, xM, xO = ring(xi, 1), ring(xi, -1), ring(xi, 2)

    def kA(s):
        return Lazy([lambda: rcopy(part.at[s, yO, :, h0], rak.at[s, 0], k_send.at[s, 0], ka.at[s, 0], yp),
                lambda: rcopy(part.at[s, yO, :, h1], rak.at[s, 1], k_send.at[s, 1], ka.at[s, 1], ym),
                lambda: rcopy(part.at[s, yP, :, h1], rbk.at[s, 0, :, h1], k_send.at[s, 2], kd.at[s, 0], yp),
                lambda: rcopy(part.at[s, yM, :, h0], rbk.at[s, 1, :, h0], k_send.at[s, 3], kd.at[s, 1], ym)])

    def kB(s):
        return Lazy([lambda: rcopy(part.at[s, yP, :, h0], rbk.at[s, 0, :, h0], k_send.at[s, 4], kb.at[s, 0], yp),
                lambda: rcopy(part.at[s, yM, :, h1], rbk.at[s, 1, :, h1], k_send.at[s, 5], kb.at[s, 1], ym)])

    def k_stepA(s):
        for a in range(2):
            t = acc[a].T
            if a == 0:
                t = t * inv_sqrt
            for y in range(4):
                part[s, y, a] = t[y * 192:(y + 1) * 192]
        for c in kA(s):
            c.start()

    def k_stepB(s):
        a = kA(s)
        b = kB(s)
        a[0].wait_recv()
        part[s, yP, :, 0:96] = part[s, yP, :, 0:96] + rak[s, 0]
        b[0].start()
        a[1].wait_recv()
        part[s, yM, :, 96:192] = part[s, yM, :, 96:192] + rak[s, 1]
        b[1].start()

    def kC(s, dc):
        o = off_out(s)
        tz, tc = ring(zi, o), core ^ dc
        return rcopy(outk.at[s, :, pl.ds(pl.multiple_of(tc * 96, 96), 96)], dkv_out.at[head], o_send.at[s, dc], ok_r.at[o, dc],
                     dev(tz, yi, xi, tc))

    def k_stepC(s):
        for c in kA(s)[2:] + kB(s):
            c.wait_recv()
        outk[s] = part[s, yi] + rbk[s, 0] + rbk[s, 1]
        kC(s, 1).start()

        @pl.when(s < 3)
        def _():
            kC(s, 0).start()

        @pl.when(s == 3)
        def _():
            dkv_out[head] = outk[s, :, pl.ds(pl.multiple_of(core * 96, 96), 96)]

    def qA(s, zq):
        return Lazy([lambda: rcopy(dq.at[zq, 0, xO], raq.at[s, 0], q_send.at[s, 0], qa.at[s, 0], xp),
                lambda: rcopy(dq.at[zq, 1, xO], raq.at[s, 1], q_send.at[s, 1], qa.at[s, 1], xm),
                lambda: rcopy(dq.at[zq, 1, xP], rbq.at[s, 0, 1], q_send.at[s, 2], qd_s.at[s, 0], xp),
                lambda: rcopy(dq.at[zq, 0, xM], rbq.at[s, 1, 0], q_send.at[s, 3], qd_s.at[s, 1], xm)])

    def qB(s, zq):
        return Lazy([lambda: rcopy(dq.at[zq, 0, xP], rbq.at[s, 0, 0], q_send.at[s, 4], qb.at[s, 0], xp),
                lambda: rcopy(dq.at[zq, 1, xM], rbq.at[s, 1, 1], q_send.at[s, 5], qb.at[s, 1], xm)])

    def zq_of(s):
        return ring(zi, off_out(s))

    def q_stepA(s):
        for c in qA(s, zq_of(s)):
            c.start()

    def q_stepB(s):
        zq = zq_of(s)
        a = qA(s, zq)
        b = qB(s, zq)
        a[0].wait_recv()
        dq[zq, 0, xP] = dq[zq, 0, xP] + raq[s, 0]
        b[0].start()
        a[1].wait_recv()
        dq[zq, 1, xM] = dq[zq, 1, xM] + raq[s, 1]
        b[1].start()

    def qC(s, dc):
        o = off_out(s)
        tz, tc = ring(zi, o), core ^ dc
        return rcopy(outq.at[s, :, tc], dq_out.at[head], o_send.at[s, 2 + dc], oq_r.at[o, dc], dev(tz, yi, xi, tc))

    def q_stepC(s):
        zq = zq_of(s)
        for c in qA(s, zq)[2:] + qB(s, zq):
            c.wait_recv()
        r = (dq[zq, :, xi] + rbq[s, 0] + rbq[s, 1]) * inv_sqrt
        outq[s] = r.astype(BF16).reshape(2, 2, 64, 128)
        qC(s, 1).start()

        @pl.when(s < 3)
        def _():
            qC(s, 0).start()

        @pl.when(s == 3)
        def _():
            dq_out[head] = outq[s, :, core]

    def pass_s(s, _):
        zk = ring(zi, off_out(s))
        acc[...] = jnp.zeros_like(acc)

        def cell_i(i, _):
            cell(zq_of(i), zk)

            @pl.when(s == 3)
            def _():
                q_stepA(i)

                @pl.when(i >= 1)
                def _():
                    q_stepB(i - 1)

                @pl.when(i >= 2)
                def _():
                    q_stepC(i - 2)

            return 0

        lax.fori_loop(0, 4, cell_i, 0)
        k_stepA(s)

        @pl.when(s >= 1)
        def _():
            k_stepB(s - 1)

        @pl.when(s >= 2)
        def _():
            k_stepC(s - 2)

        return 0

    lax.fori_loop(0, 4, pass_s, 0)
    q_stepB(3)
    k_stepB(3)
    q_stepC(2)
    k_stepC(2)
    q_stepC(3)
    k_stepC(3)

    for s in range(4):
        for dc in range(2):
            if s < 3 or dc:
                kC(s, dc).wait_recv()
                qC(s, dc).wait_recv()
    for o in offs:
        for dc in range(2):
            if o or dc:
                for c in a2a(o, dc):
                    c.wait_send()
        for c in fcopies(ring(zi, -o), o) + rcopies(ring(zi, -o), o):
            c.wait_send()
    for s in range(4):
        for c in kA(s) + kB(s) + qA(s, zq_of(s)) + qB(s, zq_of(s)):
            c.wait_send()
        for dc in range(2):
            if s < 3 or dc:
                kC(s, dc).wait_send()
                qC(s, dc).wait_send()


def solution(mesh):
    cp_size = mesh.shape['cp']
    seq_spec = P(None, 'cp', 'heads', None)
    lse_spec = P(None, 'cp', 'heads')
    kv_spec = P('cp', 'heads', None)

    def local_backward(query, attn_out, grad_out, row_lse, key_cache, value_cache):
        n_slices, rows_dev, q_heads, head_dim = query.shape
        keys_dev, kv_heads, _ = key_cache.shape
        group = q_heads // kv_heads
        grp = (n_slices, rows_dev, kv_heads, group, head_dim)
        delta = jnp.sum(grad_out.astype(F32) * attn_out.astype(F32), axis=-1)

        def by_head(a):
            return a.reshape(grp).transpose(2, 0, 1, 3, 4).reshape(kv_heads, -1, head_dim)

        def rows_by_head(a):
            return a.reshape(grp[:4]).transpose(2, 0, 1, 3).reshape(kv_heads, 1, -1)

        msg = jnp.concatenate([by_head(query), by_head(grad_out), key_cache.transpose(1, 0, 2),
                               value_cache.transpose(1, 0, 2)], axis=1)
        ld = jnp.concatenate([rows_by_head(row_lse * LOG2E), rows_by_head(delta),
                              jnp.zeros((kv_heads, 6, 128), F32)], axis=1)
        vm = pl.BlockSpec(memory_space=pltpu.VMEM)
        dma = pltpu.SemaphoreType.DMA
        shape = (n_slices, rows_dev, kv_heads, group, head_dim, keys_dev, cp_size)
        scratch = [
            pltpu.VMEM((4, 2, 2, 4, 2, 64, 128), BF16),
            pltpu.VMEM((4, 2, 4, 2, 96, 128), BF16),
            pltpu.VMEM((4, 4, 2, 8, 128), F32),
            pltpu.VMEM((4, 2, 128, 1024), BF16),
            pltpu.VMEM((4, 2, 128, 768), BF16),
            pltpu.VMEM((4, 2, 4, 128, 128), F32),
            pltpu.VMEM((4, 2, 4, 128, 128), F32),
            pltpu.VMEM((4, 2, 4, 128, 128), F32),
            pltpu.VMEM((2, 128, 768), F32),
            pltpu.VMEM((4, 4, 2, 192, 128), F32),
            pltpu.VMEM((4, 2, 2, 96, 128), F32),
            pltpu.VMEM((4, 2, 2, 192, 128), F32),
            pltpu.VMEM((4, 2, 128, 128), F32),
            pltpu.VMEM((4, 2, 2, 128, 128), F32),
            pltpu.VMEM((4, 2, 192, 128), F32),
            pltpu.VMEM((4, 2, 2, 64, 128), BF16),
            dma((8, 3)), dma((8,)), dma((8,)), dma((8,)),
            dma((4, 11)), dma((4,)), dma((4,)), dma((4,)), dma((4,)), dma((4, 3)),
            dma((4,)), dma((4,)), dma((4,)), dma((4,)),
            dma((4, 6)), dma((4, 2)), dma((4, 2)), dma((4, 2)),
            dma((4, 6)), dma((4, 2)), dma((4, 2)), dma((4, 2)),
            dma((4, 4)), dma((4, 2)), dma((4, 2)),
        ]
        dq, dkv = pl.pallas_call(
            functools.partial(kernel, shape),
            out_shape=[jax.ShapeDtypeStruct((8, 2, 64, 128), BF16), jax.ShapeDtypeStruct((8, 2, 96, 128), F32)],
            in_specs=[vm, vm], out_specs=[vm, vm], scratch_shapes=scratch,
            compiler_params=pltpu.CompilerParams(collective_id=0, has_side_effects=True, vmem_limit_bytes=60 * 2 ** 20),
            name="attn_bwd",
        )(msg, ld)
        dq = dq.reshape(kv_heads, n_slices, rows_dev, group, head_dim).transpose(1, 2, 0, 3, 4)
        dkv = dkv.transpose(1, 2, 0, 3)
        return dq.reshape(query.shape), dkv[0], dkv[1]

    return jax.shard_map(local_backward, mesh=mesh, in_specs=(seq_spec, seq_spec, seq_spec, lse_spec, kv_spec, kv_spec),
                         out_specs=(seq_spec, kv_spec, kv_spec), check_vma=False)
```

```python
import functools

import jax
import jax.numpy as jnp
from jax import lax
from jax.experimental import pallas as pl
from jax.experimental.pallas import tpu as pltpu
from jax.sharding import PartitionSpec as P

F32 = jnp.float32
BF16 = jnp.bfloat16
MESH = pl.DeviceIdType.MESH
LOG2E = 1.4426950408889634
Z = 4
HD = 128
PQ = 1024
PK = 768
TK = 256


QUERIES = "0101230123012332"
KEYS = "0011113333222200"
FORWARD_Q = ".23............."
FORWARD_K = "...32..........."
ARRIVE_Q = ".1..23.........."
ARRIVE_K = "..1...3...2....."
KC = "...........1..3."
QC = "..............01"
KB = "........1...3..2"
QB = "............01.."
QA = "..........01..32"
KA = ".....1...3...2.0"


def kernel(shape, msg, ld, dq_out, dk_out, dv_out, qd, kv, kn, ldg, qt, kt, lb, db,
           dq, acc, part, rak, rbk, raq, rbq, outk, outq,
           a_send, a_q, a_k, a_l, f_send, q_r, k_r, l_r,
           ka, kb, qa, qb, p_send, o_send, o_r):
    n_slices, rows_dev, keys_dev, head_dim, cp_size = shape
    slice_len = rows_dev * cp_size
    prefix0 = keys_dev * cp_size - n_slices * slice_len
    inv_sqrt = head_dim ** -0.5
    c2 = inv_sqrt * LOG2E
    me = lax.axis_index("cp")
    core = lax.rem(me, 2)
    xi = lax.rem(me // 2, 4)
    yi = lax.rem(me // 8, 4)
    zi = me // 32
    head = zi * 2 + core
    first = core == 0
    gq, gk = jnp.where(first, xi, yi), jnp.where(first, yi, xi)
    sq, sk = jnp.where(first, 2, 8), jnp.where(first, 8, 2)
    kbase, kstep = jnp.where(first, xi * 192, yi * PK), jnp.where(first, 576, 0)
    qbase, qstep = jnp.where(first, yi * 128, xi * 32), jnp.where(first, 0, 96)

    def ring(i, d):
        return lax.rem(i + d + 4, 4)

    qP, qM, qO = ring(gq, 1), ring(gq, -1), ring(gq, 2)
    kP, kM, kO = ring(gk, 1), ring(gk, -1), ring(gk, 2)
    dqp, dqm, dqo = me + (qP - gq) * sq, me + (qM - gq) * sq, me + (qO - gq) * sq
    dkp, dkm, dko = me + (kP - gk) * sk, me + (kM - gk) * sk, me + (kO - gk) * sk

    def dev_z(z, c):
        return z * 32 + yi * 8 + xi * 2 + c

    def off(a):
        return a ^ (a >> 1)

    def piece_z(a):
        return ring(zi, -off(a))

    def rcopy(src, dst, ss, rs, to):
        return pltpu.make_async_remote_copy(src_ref=src, dst_ref=dst, send_sem=ss, recv_sem=rs,
                                            device_id={"cp": to}, device_id_type=MESH)

    barrier = pltpu.get_barrier_semaphore()
    peers = [dqp, dqm, dqo, dkp, dkm, dko]
    for o in range(4):
        for dc in range(2):
            if o or dc:
                peers.append(dev_z(ring(zi, o), core ^ dc))
    for p in peers:
        pl.semaphore_signal(barrier, inc=1, device_id={"cp": p}, device_id_type=MESH)
    pl.semaphore_wait(barrier, len(peers))

    def got(ref, sem):
        rcopy(ref, ref, p_send.at[0], sem, me).wait_recv()

    def sent(ref, sem):
        rcopy(ref, ref, sem, l_r.at[0], me).wait_send()

    def to_head(a, dc):
        tz, tc = ring(zi, off(a)), core ^ dc
        tq, tk = jnp.where(tc == 0, xi, yi), jnp.where(tc == 0, yi, xi)
        return tz * 2 + tc, dev_z(tz, tc), tq, tk

    def q_msg(h):
        return msg.at[h, pl.ds(0, 256)].reshape(2, 2, 64, HD)

    def k_msg(h):
        return msg.at[h, pl.ds(256, 192)].reshape(2, 96, HD)

    def a2a_q(a, dc):
        h, to, tq, _ = to_head(a, dc)
        rcopy(q_msg(h), qd.at[zi, :, :, tq, core], a_send.at[0], a_q.at[a, dc], to).start()
        rcopy(ld.at[h], ldg.at[zi, tq, core], a_send.at[2], a_l.at[a], to).start()

    def a2a_k(a, dc):
        h, to, _, tk = to_head(a, dc)
        rcopy(k_msg(h), kv.at[zi, :, tk, core], a_send.at[1], a_k.at[a, dc], to).start()

    a2a_q(0, 1)
    a2a_k(0, 1)
    for f in (a2a_q, a2a_k):
        for dc in (1, 0):
            for a in (1, 2):
                f(a, dc)

    qd[zi, :, :, gq, core] = msg[head, 0:256].reshape(2, 2, 64, HD)
    kv[zi, :, gk, core] = msg[head, 256:448].reshape(2, 96, HD)
    ldg[zi, gq, core] = ld[head]

    def forward_q(a, dc):
        sz, sc = piece_z(a), core ^ dc
        c = qd.at[sz, :, :, gq, sc]
        if not (isinstance(a, int) and a == 0 and dc == 0):
            got(c, a_q.at[a, dc])
        for to in (dqp, dqm, dqo):
            rcopy(c, c, f_send.at[0], q_r.at[a], to).start()

    def forward_k(a, dc, wait=True):
        sz, sc = piece_z(a), core ^ dc
        c = kv.at[sz, :, gk, sc]
        if not (isinstance(a, int) and a == 0 and dc == 0) and wait:
            got(c, a_k.at[a, dc])
        for to in (dkp, dkm, dko):
            rcopy(c, c, f_send.at[1], k_r.at[a], to).start()

    def forward_ld(a):
        c = ldg.at[piece_z(a), gq]
        got(c.at[0] if isinstance(a, int) and a == 0 else c, a_l.at[a])
        for to in (dqp, dqm, dqo):
            rcopy(c, c, f_send.at[2], l_r.at[a], to).start()

    def arrive_q(a):
        sz = piece_z(a)
        got(qd.at[sz, :, :, 0:3], q_r.at[a])
        got(ldg.at[sz, 0:3], l_r.at[a])
        for b in range(2):
            qt[sz, b] = qd[sz, b].reshape(PQ, 128).T
        for x in range(4):
            for c in range(2):
                for ref, r in ((lb, 0), (db, 1)):
                    t = jnp.broadcast_to(ldg[sz, x, c, r:r + 1, :], (128, 128)).T
                    ref[sz, 0, x, pl.ds(c * 64, 64)] = t[:64]
                    ref[sz, 1, x, pl.ds(c * 64, 64)] = t[64:]

    def arrive_k(a):
        sz = piece_z(a)
        got(kv.at[sz, :, 0:3], k_r.at[a])
        for b in range(2):
            kt[sz, b] = kv[sz, b].reshape(PK, 128).T
        kn[sz] = kv[sz, 0].reshape(PK, 128)

    for dc in (0, 1):
        forward_q(0, dc)
        forward_k(0, dc)
    forward_ld(0)
    dq[...] = jnp.zeros_like(dq)
    acc[...] = jnp.zeros_like(acc)
    for dc in (1, 0):
        forward_q(1, dc)
    forward_ld(1)
    for dc in (1, 0):
        got(kv.at[piece_z(1), :, gk, core ^ dc], a_k.at[1, dc])
    for f in (a2a_q, a2a_k):
        for dc in (1, 0):
            f(3, dc)
    arrive_q(0)
    arrive_k(0)
    for dc in (1, 0):
        forward_k(1, dc, wait=False)

    def block(zq, zk, ak, j, tiles, masked):
        if j is None:
            rows, rsl, jsl = PQ, slice(None), slice(None)
        else:
            rows, rsl, jsl = PQ // 2, pl.ds(pl.multiple_of(j * 512, 512), 512), j
        q = qd[zq, 0, jsl].reshape(rows, HD)
        do = qd[zq, 1, jsl].reshape(rows, HD)
        lrow = jnp.concatenate([lb[zq, jsl].reshape(rows, HD)] * 2, 1)
        drow = jnp.concatenate([db[zq, jsl].reshape(rows, HD)] * 2, 1)
        if masked:
            row = lax.broadcasted_iota(jnp.int32, (rows, HD), 0)
            qrow = jnp.concatenate([(row >> 2) + (row >> 7) * qstep] * 2, 1)
            qpos = prefix0 + zq * 512 + qbase + j * slice_len

        def products(k0):
            ks = pl.ds(k0, TK)
            return (jnp.dot(q, kt[zk, 0, :, ks], preferred_element_type=F32),
                    jnp.dot(do, kt[zk, 1, :, ks], preferred_element_type=F32))

        def weights(k0, s, dp):
            p = jnp.exp2(s * c2 - lrow)
            if masked:
                kid = lax.broadcasted_iota(jnp.int32, (1, TK), 1) + k0
                run = sum((kid >= i * 192).astype(jnp.int32) for i in range(1, Z))
                kpos = zk * 3072 + kbase + kid + run * kstep
                p = jnp.where(qrow >= kpos - qpos, p, 0.0)
            return p.astype(BF16), (p * (dp - drow)).astype(BF16)

        total = None
        ahead = products(tiles[0])
        for i, k0 in enumerate(tiles):
            pb, ds = weights(k0, *ahead)
            if i + 1 < len(tiles):
                ahead = products(tiles[i + 1])
            ks = pl.ds(k0, TK)
            acc[ak, 1, :, ks] += jnp.dot(qt[zq, 1, :, rsl], pb, preferred_element_type=F32)
            acc[ak, 0, :, ks] += jnp.dot(qt[zq, 0, :, rsl], ds, preferred_element_type=F32)
            r = jnp.dot(ds, kn[zk, ks], preferred_element_type=F32)
            total = r if total is None else total + r
        dq[zq, jsl] += total.reshape((2, Z, HD, HD) if j is None else (Z, HD, HD))

    ALL = (0, TK, 2 * TK)

    def cell(zq, zk, ak):
        base = zk * 3072 + kbase
        early = prefix0 + zq * 512 + qbase
        full = base + 767 + 3 * kstep <= early

        @pl.when(full)
        def _():
            block(zq, zk, ak, None, ALL, False)

        @pl.when(jnp.logical_not(full))
        def _():
            def slice_j(j, _):
                q0 = early + j * slice_len
                last = q0 + 127 + 3 * qstep
                full_j = base + 767 + 3 * kstep <= q0
                seen2 = base + 512 + 2 * kstep <= last

                @pl.when(full_j)
                def _():
                    block(zq, zk, ak, j, ALL, False)

                @pl.when(jnp.logical_and(seen2, jnp.logical_not(full_j)))
                def _():
                    block(zq, zk, ak, j, ALL, True)

                @pl.when(jnp.logical_not(seen2))
                def _():
                    def tile_t(t, _):
                        @pl.when(base + t * (TK + kstep) <= last)
                        def _():
                            block(zq, zk, ak, j, (pl.multiple_of(t * TK, TK),), True)

                        return 0

                    lax.fori_loop(0, 2, tile_t, 0)

                return 0

            lax.fori_loop(0, 2, slice_j, 0)

    h0, h1 = pl.ds(0, 96), pl.ds(96, 96)

    def k_stepA(s):
        for b in range(2):
            t = acc[s, b].T
            if b == 0:
                t = t * inv_sqrt
            for y in range(4):
                part[s, y, b] = t[y * 192:(y + 1) * 192]
        rcopy(part.at[s, kO, :, h0], rak.at[s, 0], p_send.at[0], ka.at[s, 0], dkp).start()
        rcopy(part.at[s, kO, :, h1], rak.at[s, 1], p_send.at[0], ka.at[s, 1], dkm).start()
        rcopy(part.at[s, kP, :, h1], rbk.at[s, 0, :, h1], p_send.at[0], kb.at[s], dkp).start()
        rcopy(part.at[s, kM, :, h0], rbk.at[s, 1, :, h0], p_send.at[0], kb.at[s], dkm).start()

    def k_stepB(s):
        got(rak.at[s, 0], ka.at[s, 0])
        part[s, kP, :, 0:96] = part[s, kP, :, 0:96] + rak[s, 0]
        rcopy(part.at[s, kP, :, h0], rbk.at[s, 0, :, h0], p_send.at[0], kb.at[s], dkp).start()
        got(rak.at[s, 1], ka.at[s, 1])
        part[s, kM, :, 96:192] = part[s, kM, :, 96:192] + rak[s, 1]
        rcopy(part.at[s, kM, :, h1], rbk.at[s, 1, :, h1], p_send.at[0], kb.at[s], dkm).start()

    def k_stepC(s):
        got(rbk.at[s], kb.at[s])
        outk[s] = part[s, gk] + rbk[s, 0] + rbk[s, 1]
        tz = piece_z(s)

        def send(dc):
            tc = core ^ dc
            rows = pl.ds(pl.multiple_of(tc * 96, 96), 96)
            rcopy(outk.at[s, 0, rows], dk_out.at[head], o_send.at[0], o_r.at[0], dev_z(tz, tc)).start()
            rcopy(outk.at[s, 1, rows], dv_out.at[head], o_send.at[1], o_r.at[1], dev_z(tz, tc)).start()

        send(1)

        @pl.when(s > 0)
        def _():
            send(0)

        @pl.when(s == 0)
        def _():
            rows = pl.ds(pl.multiple_of(core * 96, 96), 96)
            dk_out[head] = outk[s, 0, rows]
            dv_out[head] = outk[s, 1, rows]

    def q_stepA(s):
        z = piece_z(s)
        rcopy(dq.at[z, 0, qO], raq.at[s, 0], p_send.at[1], qa.at[s, 0], dqp).start()
        rcopy(dq.at[z, 1, qO], raq.at[s, 1], p_send.at[1], qa.at[s, 1], dqm).start()
        rcopy(dq.at[z, 1, qP], rbq.at[s, 0, 1], p_send.at[1], qb.at[s], dqp).start()
        rcopy(dq.at[z, 0, qM], rbq.at[s, 1, 0], p_send.at[1], qb.at[s], dqm).start()

    def q_stepB(s):
        z = piece_z(s)
        got(raq.at[s, 0], qa.at[s, 0])
        dq[z, 0, qP] = dq[z, 0, qP] + raq[s, 0]
        rcopy(dq.at[z, 0, qP], rbq.at[s, 0, 0], p_send.at[1], qb.at[s], dqp).start()
        got(raq.at[s, 1], qa.at[s, 1])
        dq[z, 1, qM] = dq[z, 1, qM] + raq[s, 1]
        rcopy(dq.at[z, 1, qM], rbq.at[s, 1, 1], p_send.at[1], qb.at[s], dqm).start()

    def q_stepC(s):
        z = piece_z(s)
        got(rbq.at[s], qb.at[s])
        r = (dq[z, :, gq] + rbq[s, 0] + rbq[s, 1]) * inv_sqrt
        outq[s] = r.astype(BF16).reshape(2, 2, 64, 128)

        def send(dc):
            tc = core ^ dc
            rcopy(outq.at[s, :, tc], dq_out.at[head], o_send.at[2], o_r.at[2], dev_z(z, tc)).start()

        send(1)

        @pl.when(s > 0)
        def _():
            send(0)

        @pl.when(s == 0)
        def _():
            dq_out[head] = outq[s, :, core]

    def word(digits, bits):
        v = sum(int(d) << (bits * i) for i, d in enumerate(digits))
        return jnp.int32(v - (1 << 32) if v >> 31 else v)

    def pick(table, n):
        return (word(table.replace(".", "0"), 2) >> (2 * n)) & 3

    def hit(tables, n):
        on = "".join("1" if any(t[i] != "." for t in tables) else "0" for i in range(16))
        return ((word(on, 1) >> n) & 1) == 1

    def at(table, n, f):
        @pl.when(hit([table], n))
        def _():
            f(pick(table, n))

    def both(f, last=None):
        def g(a):
            f(a, 1)
            f(a, 0)
            if last is not None:
                last(a)

        return g

    def group(parts, n):
        @pl.when(hit([t for t, _ in parts], n))
        def _():
            for t, f in parts:
                at(t, n, f)

    def step(n, _):
        group(((FORWARD_Q, both(forward_q, forward_ld)), (FORWARD_K, both(forward_k)),
               (ARRIVE_Q, arrive_q), (ARRIVE_K, arrive_k)), n)
        aq, ak = pick(QUERIES, n), pick(KEYS, n)
        cell(piece_z(aq), piece_z(ak), ak)
        group(((KC, k_stepC), (QC, q_stepC), (KB, k_stepB), (QB, q_stepB), (QA, q_stepA), (KA, k_stepA)), n)
        return 0

    lax.fori_loop(0, 16, step, 0)
    one = jnp.int32
    q_stepB(one(3))
    q_stepB(one(2))
    k_stepB(one(0))
    k_stepC(one(2))
    q_stepC(one(3))
    q_stepC(one(2))
    k_stepC(one(0))

    got(dk_out.at[0:7], o_r.at[0])
    got(dv_out.at[0:7], o_r.at[1])
    got(dq_out.at[0:7], o_r.at[2])
    sent(msg.at[0:7, pl.ds(0, 256)], a_send.at[0])
    sent(msg.at[0:7, pl.ds(256, 192)], a_send.at[1])
    sent(ld.at[0:7], a_send.at[2])
    sent(qd.at[0:3], f_send.at[0])
    sent(kv.at[0:3], f_send.at[1])
    sent(ldg.at[0:3], f_send.at[2])
    sent(part.at[0:3], p_send.at[0])
    sent(dq.at[0:3], p_send.at[1])
    sent(dk_out.at[0:7], o_send.at[0])
    sent(dv_out.at[0:7], o_send.at[1])
    sent(dq_out.at[0:7], o_send.at[2])


def solution(mesh):
    cp_size = mesh.shape['cp']
    seq_spec = P(None, 'cp', 'heads', None)
    lse_spec = P(None, 'cp', 'heads')
    kv_spec = P('cp', 'heads', None)

    def local_backward(query, attn_out, grad_out, row_lse, key_cache, value_cache):
        n_slices, rows_dev, q_heads, head_dim = query.shape
        keys_dev, kv_heads, _ = key_cache.shape
        group = q_heads // kv_heads
        grp = (n_slices, rows_dev, kv_heads, group, head_dim)
        delta = jnp.sum(grad_out.astype(F32) * attn_out.astype(F32), axis=-1)

        def by_head(a):
            return a.reshape(grp).transpose(2, 0, 1, 3, 4).reshape(kv_heads, -1, head_dim)

        def rows_by_head(a):
            return a.reshape(grp[:4]).transpose(2, 0, 1, 3).reshape(kv_heads, 1, -1)

        ld = jnp.concatenate([rows_by_head(row_lse * LOG2E), rows_by_head(delta),
                              jnp.zeros((kv_heads, 6, 128), F32)], axis=1)
        msg = jnp.concatenate([by_head(query), by_head(grad_out), key_cache.transpose(1, 0, 2),
                               value_cache.transpose(1, 0, 2)], axis=1)
        vm = pl.BlockSpec(memory_space=pltpu.VMEM)
        dma = pltpu.SemaphoreType.DMA
        shape = (n_slices, rows_dev, keys_dev, head_dim, cp_size)
        scratch = [
            pltpu.VMEM((Z, 2, 2, Z, 2, 64, HD), BF16),
            pltpu.VMEM((Z, 2, Z, 2, 96, HD), BF16),
            pltpu.VMEM((Z, PK, HD), BF16),
            pltpu.VMEM((Z, Z, 2, 8, HD), F32),
            pltpu.VMEM((Z, 2, HD, PQ), BF16),
            pltpu.VMEM((Z, 2, HD, PK), BF16),
            pltpu.VMEM((Z, 2, Z, HD, HD), F32),
            pltpu.VMEM((Z, 2, Z, HD, HD), F32),
            pltpu.VMEM((Z, 2, Z, HD, HD), F32),
            pltpu.VMEM((Z, 2, HD, PK), F32),
            pltpu.VMEM((Z, Z, 2, 192, HD), F32),
            pltpu.VMEM((Z, 2, 2, 96, HD), F32),
            pltpu.VMEM((Z, 2, 2, 192, HD), F32),
            pltpu.VMEM((Z, 2, HD, HD), F32),
            pltpu.VMEM((Z, 2, 2, HD, HD), F32),
            pltpu.VMEM((Z, 2, 192, HD), F32),
            pltpu.VMEM((Z, 2, 2, 64, HD), BF16),
            dma((3,)), dma((4, 2)), dma((4, 2)), dma((Z,)),
            dma((3,)), dma((Z,)), dma((Z,)), dma((Z,)),
            dma((4, 2)), dma((Z,)), dma((4, 2)), dma((Z,)),
            dma((2,)), dma((3,)), dma((3,)),
        ]
        dq, dk, dv = pl.pallas_call(
            functools.partial(kernel, shape),
            out_shape=[jax.ShapeDtypeStruct((8, 2, 64, 128), BF16), jax.ShapeDtypeStruct((8, 96, 128), F32),
                       jax.ShapeDtypeStruct((8, 96, 128), F32)],
            in_specs=[vm] * 2, out_specs=[vm] * 3, scratch_shapes=scratch,
            compiler_params=pltpu.CompilerParams(collective_id=0, has_side_effects=True, vmem_limit_bytes=46 * 2 ** 20),
            name="attn_bwd",
        )(msg, ld)
        dq = dq.reshape(kv_heads, n_slices, rows_dev, group, head_dim).transpose(1, 2, 0, 3, 4)
        return dq.reshape(query.shape), dk.transpose(1, 0, 2), dv.transpose(1, 0, 2)

    return jax.shard_map(local_backward, mesh=mesh, in_specs=(seq_spec, seq_spec, seq_spec, lse_spec, kv_spec, kv_spec),
                         out_specs=(seq_spec, kv_spec, kv_spec), check_vma=False)
```

```python
import functools

import jax
import jax.numpy as jnp
from jax import lax
from jax.experimental import pallas as pl
from jax.experimental.pallas import tpu as pltpu
from jax.sharding import PartitionSpec as P

F32 = jnp.float32
BF16 = jnp.bfloat16
MESH = pl.DeviceIdType.MESH
LOG2E = 1.4426950408889634
Z = 4
HD = 128
PQ = 1024
PK = 768
TK = 256


QUERIES = "0101230123012332"
KEYS = "0011113333222200"
FORWARD_Q = ".23............."
FORWARD_K = "...32..........."
ARRIVE_Q = ".1..23.........."
ARRIVE_K = "..1...3...2....."
KC = "...........1..3."
QC = "..............01"
KB = "........1...3..2"
QB = "............01.."
QA = "..........01..32"
KA = ".....1...3...2.0"


def kernel(shape, query, attn_out, grad_out, row_lse, key_cache, value_cache, dq_out, dk_out, dv_out,
           in_q, in_o, in_do, in_lse, in_k, in_v, rows32, msg, ld, in_sems, qd, kv, kn, ldg, qt, kt, lb, db,
           dq, acc, part, rak, rbk, raq, rbq, outk, outq,
           a_send, a_q, a_k, a_l, f_send, q_r, k_r, l_r,
           ka, kb, qa, qb, p_send, o_send, o_r):
    n_slices, rows_dev, keys_dev, head_dim, cp_size = shape
    slice_len = rows_dev * cp_size
    prefix0 = keys_dev * cp_size - n_slices * slice_len
    inv_sqrt = head_dim ** -0.5
    c2 = inv_sqrt * LOG2E
    me = lax.axis_index("cp")
    core = lax.rem(me, 2)
    xi = lax.rem(me // 2, 4)
    yi = lax.rem(me // 8, 4)
    zi = me // 32
    head = zi * 2 + core
    first = core == 0
    gq, gk = jnp.where(first, xi, yi), jnp.where(first, yi, xi)
    sq, sk = jnp.where(first, 2, 8), jnp.where(first, 8, 2)
    kbase, kstep = jnp.where(first, xi * 192, yi * PK), jnp.where(first, 576, 0)
    qbase, qstep = jnp.where(first, yi * 128, xi * 32), jnp.where(first, 0, 96)

    def ring(i, d):
        return lax.rem(i + d + 4, 4)

    qP, qM, qO = ring(gq, 1), ring(gq, -1), ring(gq, 2)
    kP, kM, kO = ring(gk, 1), ring(gk, -1), ring(gk, 2)
    dqp, dqm, dqo = me + (qP - gq) * sq, me + (qM - gq) * sq, me + (qO - gq) * sq
    dkp, dkm, dko = me + (kP - gk) * sk, me + (kM - gk) * sk, me + (kO - gk) * sk

    def dev_z(z, c):
        return z * 32 + yi * 8 + xi * 2 + c

    def off(a):
        return a ^ (a >> 1)

    def piece_z(a):
        return ring(zi, -off(a))

    def rcopy(src, dst, ss, rs, to):
        return pltpu.make_async_remote_copy(src_ref=src, dst_ref=dst, send_sem=ss, recv_sem=rs,
                                            device_id={"cp": to}, device_id_type=MESH)

    inputs = [pltpu.make_async_copy(src, dst, in_sems.at[i]) for i, (src, dst) in enumerate((
        (query, in_q), (grad_out, in_do), (key_cache, in_k), (value_cache, in_v), (attn_out, in_o), (row_lse, in_lse)))]
    for c in inputs:
        c.start()

    barrier = pltpu.get_barrier_semaphore()
    peers = [dqp, dqm, dqo, dkp, dkm, dko]
    for o in range(4):
        for dc in range(2):
            if o or dc:
                peers.append(dev_z(ring(zi, o), core ^ dc))
    for p in peers:
        pl.semaphore_signal(barrier, inc=1, device_id={"cp": p}, device_id_type=MESH)

    def rows_of(ref, h):
        return ref[:, :, h].astype(F32).reshape(128, HD)

    for c in inputs[:2]:
        c.wait()
    for h in range(8):
        msg[h, 0:128] = rows_of(in_q, h).astype(BF16)
        msg[h, 128:256] = rows_of(in_do, h).astype(BF16)
    pl.semaphore_wait(barrier, len(peers))

    def got(ref, sem):
        rcopy(ref, ref, p_send.at[0], sem, me).wait_recv()

    def sent(ref, sem):
        rcopy(ref, ref, sem, l_r.at[0], me).wait_send()

    def to_head(a, dc):
        tz, tc = ring(zi, off(a)), core ^ dc
        tq, tk = jnp.where(tc == 0, xi, yi), jnp.where(tc == 0, yi, xi)
        return tz * 2 + tc, dev_z(tz, tc), tq, tk

    def q_msg(h):
        return msg.at[h, pl.ds(0, 256)].reshape(2, 2, 64, HD)

    def k_msg(h):
        return msg.at[h, pl.ds(256, 192)].reshape(2, 96, HD)

    def a2a_q(a, dc):
        h, to, tq, _ = to_head(a, dc)
        rcopy(q_msg(h), qd.at[zi, :, :, tq, core], a_send.at[0], a_q.at[a, dc], to).start()

    def a2a_ld(a, dc):
        h, to, tq, _ = to_head(a, dc)
        rcopy(ld.at[h], ldg.at[zi, tq, core], a_send.at[2], a_l.at[a], to).start()

    def a2a_k(a, dc):
        h, to, _, tk = to_head(a, dc)
        rcopy(k_msg(h), kv.at[zi, :, tk, core], a_send.at[1], a_k.at[a, dc], to).start()

    def forward_q(a, dc):
        sz, sc = piece_z(a), core ^ dc
        c = qd.at[sz, :, :, gq, sc]
        if not (isinstance(a, int) and a == 0 and dc == 0):
            got(c, a_q.at[a, dc])
        for to in (dqp, dqm, dqo):
            rcopy(c, c, f_send.at[0], q_r.at[a], to).start()

    def forward_k(a, dc, wait=True):
        sz, sc = piece_z(a), core ^ dc
        c = kv.at[sz, :, gk, sc]
        if not (isinstance(a, int) and a == 0 and dc == 0) and wait:
            got(c, a_k.at[a, dc])
        for to in (dkp, dkm, dko):
            rcopy(c, c, f_send.at[1], k_r.at[a], to).start()

    def forward_ld(a):
        c = ldg.at[piece_z(a), gq]
        got(c.at[0] if isinstance(a, int) and a == 0 else c, a_l.at[a])
        for to in (dqp, dqm, dqo):
            rcopy(c, c, f_send.at[2], l_r.at[a], to).start()

    def arrive_q(a):
        sz = piece_z(a)
        got(qd.at[sz, :, :, 0:3], q_r.at[a])
        got(ldg.at[sz, 0:3], l_r.at[a])
        for b in range(2):
            qt[sz, b] = qd[sz, b].reshape(PQ, 128).T
        for x in range(4):
            for c in range(2):
                for ref, r in ((lb, 0), (db, 1)):
                    t = jnp.broadcast_to(ldg[sz, x, c, r:r + 1, :], (128, 128)).T
                    ref[sz, 0, x, pl.ds(c * 64, 64)] = t[:64]
                    ref[sz, 1, x, pl.ds(c * 64, 64)] = t[64:]

    def arrive_k(a):
        sz = piece_z(a)
        got(kv.at[sz, :, 0:3], k_r.at[a])
        for b in range(2):
            kt[sz, b] = kv[sz, b].reshape(PK, 128).T
        kn[sz] = kv[sz, 0].reshape(PK, 128)

    a2a_q(0, 1)
    for dc in (1, 0):
        for a in (1, 2):
            a2a_q(a, dc)
    qd[zi, :, :, gq, core] = msg[head, 0:256].reshape(2, 2, 64, HD)
    forward_q(0, 0)
    for c, ref, r in ((inputs[2], in_k, 256), (inputs[3], in_v, 352)):
        c.wait()
        rows32[...] = ref[...].astype(F32)
        for h in range(8):
            msg[h, r:r + 96] = rows32[:, h, :].astype(BF16)
    a2a_k(0, 1)
    for dc in (1, 0):
        for a in (1, 2):
            a2a_k(a, dc)
    kv[zi, :, gk, core] = msg[head, 256:448].reshape(2, 96, HD)
    forward_k(0, 0)
    forward_q(0, 1)
    forward_k(0, 1)

    for c in inputs[4:]:
        c.wait()
    row = lax.broadcasted_iota(jnp.int32, (128, HD), 0)
    lane = lax.broadcasted_iota(jnp.int32, (128, HD), 1)
    lse = jnp.concatenate([in_lse[...].reshape(32, 32) * LOG2E, jnp.zeros((32, 96), F32)], 1)
    lse = jnp.broadcast_to(lse.reshape(32, 1, HD), (32, Z, HD)).reshape(128, HD)
    ld[...] = jnp.zeros_like(ld)
    for h in range(8):
        one = jnp.where(lane == Z * h + (row & 3), lse, 0.0)
        ld[h, 0:1] = jnp.sum(one.T, axis=0, keepdims=True)
        ld[h, 1:2] = jnp.sum((rows_of(in_do, h) * rows_of(in_o, h)).T, axis=0, keepdims=True)
    a2a_ld(0, 1)
    for dc in (1, 0):
        for a in (1, 2):
            a2a_ld(a, dc)
    ldg[zi, gq, core] = ld[head]
    forward_ld(0)
    dq[...] = jnp.zeros_like(dq)
    acc[...] = jnp.zeros_like(acc)
    for dc in (1, 0):
        forward_q(1, dc)
    forward_ld(1)
    for dc in (1, 0):
        got(kv.at[piece_z(1), :, gk, core ^ dc], a_k.at[1, dc])
    for f in (a2a_q, a2a_k, a2a_ld):
        for dc in (1, 0):
            f(3, dc)
    arrive_q(0)
    arrive_k(0)
    for dc in (1, 0):
        forward_k(1, dc, wait=False)

    def block(zq, zk, ak, j, tiles, masked):
        if j is None:
            rows, rsl, jsl = PQ, slice(None), slice(None)
        else:
            rows, rsl, jsl = PQ // 2, pl.ds(pl.multiple_of(j * 512, 512), 512), j
        q = qd[zq, 0, jsl].reshape(rows, HD)
        do = qd[zq, 1, jsl].reshape(rows, HD)
        lrow = jnp.concatenate([lb[zq, jsl].reshape(rows, HD)] * 2, 1)
        drow = jnp.concatenate([db[zq, jsl].reshape(rows, HD)] * 2, 1)
        if masked:
            row = lax.broadcasted_iota(jnp.int32, (rows, HD), 0)
            qrow = jnp.concatenate([(row >> 2) + (row >> 7) * qstep] * 2, 1)
            qpos = prefix0 + zq * 512 + qbase + j * slice_len

        def products(k0):
            ks = pl.ds(k0, TK)
            return (jnp.dot(q, kt[zk, 0, :, ks], preferred_element_type=F32),
                    jnp.dot(do, kt[zk, 1, :, ks], preferred_element_type=F32))

        def weights(k0, s, dp):
            p = jnp.exp2(s * c2 - lrow)
            if masked:
                kid = lax.broadcasted_iota(jnp.int32, (1, TK), 1) + k0
                run = sum((kid >= i * 192).astype(jnp.int32) for i in range(1, Z))
                kpos = zk * 3072 + kbase + kid + run * kstep
                p = jnp.where(qrow >= kpos - qpos, p, 0.0)
            return p.astype(BF16), (p * (dp - drow)).astype(BF16)

        total = None
        ahead = products(tiles[0])
        for i, k0 in enumerate(tiles):
            pb, ds = weights(k0, *ahead)
            if i + 1 < len(tiles):
                ahead = products(tiles[i + 1])
            ks = pl.ds(k0, TK)
            acc[ak, 1, :, ks] += jnp.dot(qt[zq, 1, :, rsl], pb, preferred_element_type=F32)
            acc[ak, 0, :, ks] += jnp.dot(qt[zq, 0, :, rsl], ds, preferred_element_type=F32)
            r = jnp.dot(ds, kn[zk, ks], preferred_element_type=F32)
            total = r if total is None else total + r
        dq[zq, jsl] += total.reshape((2, Z, HD, HD) if j is None else (Z, HD, HD))

    ALL = (0, TK, 2 * TK)

    def cell(zq, zk, ak):
        base = zk * 3072 + kbase
        early = prefix0 + zq * 512 + qbase
        full = base + 767 + 3 * kstep <= early

        @pl.when(full)
        def _():
            block(zq, zk, ak, None, ALL, False)

        @pl.when(jnp.logical_not(full))
        def _():
            def slice_j(j, _):
                q0 = early + j * slice_len
                last = q0 + 127 + 3 * qstep
                full_j = base + 767 + 3 * kstep <= q0
                seen2 = base + 512 + 2 * kstep <= last

                @pl.when(full_j)
                def _():
                    block(zq, zk, ak, j, ALL, False)

                @pl.when(jnp.logical_and(seen2, jnp.logical_not(full_j)))
                def _():
                    block(zq, zk, ak, j, ALL, True)

                @pl.when(jnp.logical_not(seen2))
                def _():
                    def tile_t(t, _):
                        @pl.when(base + t * (TK + kstep) <= last)
                        def _():
                            block(zq, zk, ak, j, (pl.multiple_of(t * TK, TK),), True)

                        return 0

                    lax.fori_loop(0, 2, tile_t, 0)

                return 0

            lax.fori_loop(0, 2, slice_j, 0)

    h0, h1 = pl.ds(0, 96), pl.ds(96, 96)

    def k_stepA(s):
        for b in range(2):
            t = acc[s, b].T
            if b == 0:
                t = t * inv_sqrt
            for y in range(4):
                part[s, y, b] = t[y * 192:(y + 1) * 192]
        rcopy(part.at[s, kO, :, h0], rak.at[s, 0], p_send.at[0], ka.at[s, 0], dkp).start()
        rcopy(part.at[s, kO, :, h1], rak.at[s, 1], p_send.at[0], ka.at[s, 1], dkm).start()
        rcopy(part.at[s, kP, :, h1], rbk.at[s, 0, :, h1], p_send.at[0], kb.at[s], dkp).start()
        rcopy(part.at[s, kM, :, h0], rbk.at[s, 1, :, h0], p_send.at[0], kb.at[s], dkm).start()

    def k_stepB(s):
        got(rak.at[s, 0], ka.at[s, 0])
        part[s, kP, :, 0:96] = part[s, kP, :, 0:96] + rak[s, 0]
        rcopy(part.at[s, kP, :, h0], rbk.at[s, 0, :, h0], p_send.at[0], kb.at[s], dkp).start()
        got(rak.at[s, 1], ka.at[s, 1])
        part[s, kM, :, 96:192] = part[s, kM, :, 96:192] + rak[s, 1]
        rcopy(part.at[s, kM, :, h1], rbk.at[s, 1, :, h1], p_send.at[0], kb.at[s], dkm).start()

    def k_stepC(s):
        got(rbk.at[s], kb.at[s])
        outk[s] = part[s, gk] + rbk[s, 0] + rbk[s, 1]
        tz = piece_z(s)

        def send(dc):
            tc = core ^ dc
            rows = pl.ds(pl.multiple_of(tc * 96, 96), 96)
            rcopy(outk.at[s, 0, rows], dk_out.at[head], o_send.at[0], o_r.at[0], dev_z(tz, tc)).start()
            rcopy(outk.at[s, 1, rows], dv_out.at[head], o_send.at[1], o_r.at[1], dev_z(tz, tc)).start()

        send(1)

        @pl.when(s > 0)
        def _():
            send(0)

        @pl.when(s == 0)
        def _():
            rows = pl.ds(pl.multiple_of(core * 96, 96), 96)
            dk_out[head] = outk[s, 0, rows]
            dv_out[head] = outk[s, 1, rows]

    def q_stepA(s):
        z = piece_z(s)
        rcopy(dq.at[z, 0, qO], raq.at[s, 0], p_send.at[1], qa.at[s, 0], dqp).start()
        rcopy(dq.at[z, 1, qO], raq.at[s, 1], p_send.at[1], qa.at[s, 1], dqm).start()
        rcopy(dq.at[z, 1, qP], rbq.at[s, 0, 1], p_send.at[1], qb.at[s], dqp).start()
        rcopy(dq.at[z, 0, qM], rbq.at[s, 1, 0], p_send.at[1], qb.at[s], dqm).start()

    def q_stepB(s):
        z = piece_z(s)
        got(raq.at[s, 0], qa.at[s, 0])
        dq[z, 0, qP] = dq[z, 0, qP] + raq[s, 0]
        rcopy(dq.at[z, 0, qP], rbq.at[s, 0, 0], p_send.at[1], qb.at[s], dqp).start()
        got(raq.at[s, 1], qa.at[s, 1])
        dq[z, 1, qM] = dq[z, 1, qM] + raq[s, 1]
        rcopy(dq.at[z, 1, qM], rbq.at[s, 1, 1], p_send.at[1], qb.at[s], dqm).start()

    def q_stepC(s):
        z = piece_z(s)
        got(rbq.at[s], qb.at[s])
        r = (dq[z, :, gq] + rbq[s, 0] + rbq[s, 1]) * inv_sqrt
        outq[s] = r.reshape(2, 2, 16, 4, HD).astype(BF16)

        def send(dc):
            tc = core ^ dc
            rcopy(outq.at[s, :, tc], dq_out.at[:, :, head], o_send.at[2], o_r.at[2], dev_z(z, tc)).start()

        send(1)

        @pl.when(s > 0)
        def _():
            send(0)

        @pl.when(s == 0)
        def _():
            dq_out[:, :, head] = outq[s, :, core]

    def word(digits, bits):
        v = sum(int(d) << (bits * i) for i, d in enumerate(digits))
        return jnp.int32(v - (1 << 32) if v >> 31 else v)

    def pick(table, n):
        return (word(table.replace(".", "0"), 2) >> (2 * n)) & 3

    def hit(tables, n):
        on = "".join("1" if any(t[i] != "." for t in tables) else "0" for i in range(16))
        return ((word(on, 1) >> n) & 1) == 1

    def at(table, n, f):
        @pl.when(hit([table], n))
        def _():
            f(pick(table, n))

    def both(f, last=None):
        def g(a):
            f(a, 1)
            f(a, 0)
            if last is not None:
                last(a)

        return g

    def group(parts, n):
        @pl.when(hit([t for t, _ in parts], n))
        def _():
            for t, f in parts:
                at(t, n, f)

    def step(n, _):
        group(((FORWARD_Q, both(forward_q, forward_ld)), (FORWARD_K, both(forward_k)),
               (ARRIVE_Q, arrive_q), (ARRIVE_K, arrive_k)), n)
        aq, ak = pick(QUERIES, n), pick(KEYS, n)
        cell(piece_z(aq), piece_z(ak), ak)
        group(((KC, k_stepC), (QC, q_stepC), (KB, k_stepB), (QB, q_stepB), (QA, q_stepA), (KA, k_stepA)), n)
        return 0

    lax.fori_loop(0, 16, step, 0)
    one = jnp.int32
    q_stepB(one(3))
    q_stepB(one(2))
    k_stepB(one(0))
    k_stepC(one(2))
    q_stepC(one(3))
    q_stepC(one(2))
    k_stepC(one(0))

    got(dk_out.at[0:7], o_r.at[0])
    got(dv_out.at[0:7], o_r.at[1])
    got(dq_out.at[:, :, 0:7], o_r.at[2])
    sent(msg.at[0:7, pl.ds(0, 256)], a_send.at[0])
    sent(msg.at[0:7, pl.ds(256, 192)], a_send.at[1])
    sent(ld.at[0:7], a_send.at[2])
    sent(qd.at[0:3], f_send.at[0])
    sent(kv.at[0:3], f_send.at[1])
    sent(ldg.at[0:3], f_send.at[2])
    sent(part.at[0:3], p_send.at[0])
    sent(dq.at[0:3], p_send.at[1])
    sent(dk_out.at[0:7], o_send.at[0])
    sent(dv_out.at[0:7], o_send.at[1])
    sent(dq_out.at[:, :, 0:7], o_send.at[2])


def store_kernel(dq, dk, dv, dq_out, dk_out, dv_out, dk_rows, dv_rows, sems):
    copies = [pltpu.make_async_copy(dq, dq_out, sems.at[0]), pltpu.make_async_copy(dk_rows, dk_out, sems.at[1]),
              pltpu.make_async_copy(dv_rows, dv_out, sems.at[2])]
    copies[0].start()
    for x, rows, c in ((dk, dk_rows, copies[1]), (dv, dv_rows, copies[2])):
        for h in range(8):
            rows[:, h, :] = x[h]
        c.start()
    for c in copies:
        c.wait()


def solution(mesh):
    cp_size = mesh.shape['cp']
    seq_spec = P(None, 'cp', 'heads', None)
    lse_spec = P(None, 'cp', 'heads')
    kv_spec = P('cp', 'heads', None)

    def local_backward(query, attn_out, grad_out, row_lse, key_cache, value_cache):
        n_slices, rows_dev, q_heads, head_dim = query.shape
        keys_dev, kv_heads, _ = key_cache.shape
        group = q_heads // kv_heads
        grp = (n_slices, rows_dev, kv_heads, group, head_dim)
        vm = pl.BlockSpec(memory_space=pltpu.VMEM)
        dma = pltpu.SemaphoreType.DMA
        shape = (n_slices, rows_dev, keys_dev, head_dim, cp_size)
        scratch = [
            pltpu.VMEM(grp, BF16),
            pltpu.VMEM(grp, BF16),
            pltpu.VMEM(grp, BF16),
            pltpu.VMEM(row_lse.shape, F32),
            pltpu.VMEM(key_cache.shape, BF16),
            pltpu.VMEM(key_cache.shape, BF16),
            pltpu.VMEM(key_cache.shape, F32),
            pltpu.VMEM((8, 448, HD), BF16),
            pltpu.VMEM((8, 8, HD), F32),
            dma((6,)),
            pltpu.VMEM((Z, 2, 2, Z, 2, 64, HD), BF16),
            pltpu.VMEM((Z, 2, Z, 2, 96, HD), BF16),
            pltpu.VMEM((Z, PK, HD), BF16),
            pltpu.VMEM((Z, Z, 2, 8, HD), F32),
            pltpu.VMEM((Z, 2, HD, PQ), BF16),
            pltpu.VMEM((Z, 2, HD, PK), BF16),
            pltpu.VMEM((Z, 2, Z, HD, HD), F32),
            pltpu.VMEM((Z, 2, Z, HD, HD), F32),
            pltpu.VMEM((Z, 2, Z, HD, HD), F32),
            pltpu.VMEM((Z, 2, HD, PK), F32),
            pltpu.VMEM((Z, Z, 2, 192, HD), F32),
            pltpu.VMEM((Z, 2, 2, 96, HD), F32),
            pltpu.VMEM((Z, 2, 2, 192, HD), F32),
            pltpu.VMEM((Z, 2, HD, HD), F32),
            pltpu.VMEM((Z, 2, 2, HD, HD), F32),
            pltpu.VMEM((Z, 2, 192, HD), F32),
            pltpu.VMEM((Z, 2, 2, 16, 4, HD), BF16),
            dma((3,)), dma((4, 2)), dma((4, 2)), dma((Z,)),
            dma((3,)), dma((Z,)), dma((Z,)), dma((Z,)),
            dma((4, 2)), dma((Z,)), dma((4, 2)), dma((Z,)),
            dma((2,)), dma((3,)), dma((3,)),
        ]
        dq, dk, dv = pl.pallas_call(
            functools.partial(kernel, shape),
            out_shape=[jax.ShapeDtypeStruct(grp, BF16), jax.ShapeDtypeStruct((8, 96, HD), F32),
                       jax.ShapeDtypeStruct((8, 96, HD), F32)],
            in_specs=[pl.BlockSpec(memory_space=pltpu.HBM)] * 6, out_specs=[vm] * 3, scratch_shapes=scratch,
            compiler_params=pltpu.CompilerParams(collective_id=0, has_side_effects=True, vmem_limit_bytes=46 * 2 ** 20),
            name="attn_bwd",
        )(*(pltpu.with_memory_space_constraint(a, pltpu.HBM) for a in (query.reshape(grp), attn_out.reshape(grp), grad_out.reshape(grp), row_lse, key_cache, value_cache)))
        hbm = pl.BlockSpec(memory_space=pl.ANY)
        dq, dk, dv = pl.pallas_call(
            store_kernel,
            out_shape=[jax.ShapeDtypeStruct(dq.shape, BF16), jax.ShapeDtypeStruct(key_cache.shape, F32),
                       jax.ShapeDtypeStruct(key_cache.shape, F32)],
            in_specs=[vm] * 3, out_specs=[hbm] * 3,
            scratch_shapes=[pltpu.VMEM(key_cache.shape, F32), pltpu.VMEM(key_cache.shape, F32), dma((3,))],
            compiler_params=pltpu.CompilerParams(vmem_limit_bytes=2 ** 22), name="store",
        )(dq, dk, dv)
        return dq.reshape(query.shape), dk, dv

    return jax.shard_map(local_backward, mesh=mesh, in_specs=(seq_spec, seq_spec, seq_spec, lse_spec, kv_spec, kv_spec),
                         out_specs=(seq_spec, kv_spec, kv_spec), check_vma=False)
```

```python
import functools

import jax
import jax.numpy as jnp
from jax import lax
from jax.experimental import pallas as pl
from jax.experimental.pallas import tpu as pltpu
from jax.sharding import PartitionSpec as P

F32 = jnp.float32
BF16 = jnp.bfloat16
MESH = pl.DeviceIdType.MESH
LOG2E = 1.4426950408889634
Z = 4
HD = 128
PQ = 1024
PK = 768
TK = 256
KR = 96
QR = 64


QUERIES = "1012301230123320"
KEYS = "0111133332222000"
FORWARD_Q = ".3.............."
FORWARD_K = "..3..2.........."
ARRIVE_Q = "1..23..........."
ARRIVE_K = ".1...3...2......"
KC = ".............1.3"
QC = "...............1"
KB = ".......1...3..2."
QB = "...........01..."
RB = "................"
QA = ".........01..32."
RA = "...............0"
KA = "....1...3...2..0"
LAST = "qB3qB2kC2qC3rB0kB0qC2qC0kC0"


def kernel(shape, query, attn_out, grad_out, row_lse, key_cache, value_cache, dq_out, dk_out, dv_out,
           in_q, in_o, in_do, in_lse, in_k, in_v, rows32, msg, ld, in_sems, spread, qd, kv, kn, ldg, qt, kt, lb, db,
           dq, acc, part, rak, rbk, raq, rbq, outk, outq,
           a_send, a_q, a_k, a_l, f_send, q_r, k_r, l_r,
           ka, kb, qa, qb, p_send, o_send, o_r):
    n_slices, rows_dev, keys_dev, head_dim, cp_size = shape
    slice_len = rows_dev * cp_size
    prefix0 = keys_dev * cp_size - n_slices * slice_len
    inv_sqrt = head_dim ** -0.5
    c2 = inv_sqrt * LOG2E
    me = lax.axis_index("cp")
    core = lax.rem(me, 2)
    xi = lax.rem(me // 2, 4)
    yi = lax.rem(me // 8, 4)
    zi = me // 32
    head = zi * 2 + core
    first = core == 0
    gq, gk = jnp.where(first, xi, yi), jnp.where(first, yi, xi)
    sq, sk = jnp.where(first, 2, 8), jnp.where(first, 8, 2)
    kbase, kstep = jnp.where(first, xi * 192, yi * PK), jnp.where(first, 576, 0)
    qbase, qstep = jnp.where(first, yi * 128, xi * 32), jnp.where(first, 0, 96)

    def ring(i, d):
        return lax.rem(i + d + 4, 4)

    qP, qM, qO = ring(gq, 1), ring(gq, -1), ring(gq, 2)
    kP, kM, kO = ring(gk, 1), ring(gk, -1), ring(gk, 2)
    dqp, dqm, dqo = me + (qP - gq) * sq, me + (qM - gq) * sq, me + (qO - gq) * sq
    dkp, dkm, dko = me + (kP - gk) * sk, me + (kM - gk) * sk, me + (kO - gk) * sk

    def dev_z(z, c):
        return z * 32 + yi * 8 + xi * 2 + c

    def off(a, c):
        o = a ^ (a >> 1)
        return jnp.where(c == 0, o, (Z - o) & 3)

    def piece_z(a):
        return ring(zi, -off(a, core))

    def rcopy(src, dst, ss, rs, to):
        return pltpu.make_async_remote_copy(src_ref=src, dst_ref=dst, send_sem=ss, recv_sem=rs,
                                            device_id={"cp": to}, device_id_type=MESH)

    inputs = [pltpu.make_async_copy(src, dst, in_sems.at[i]) for i, (src, dst) in enumerate((
        (query, in_q), (grad_out, in_do), (key_cache, in_k), (value_cache, in_v), (attn_out, in_o), (row_lse, in_lse)))]
    for c in inputs:
        c.start()

    barrier = pltpu.get_barrier_semaphore()
    peers = [dqp, dqm, dqo, dkp, dkm, dko]
    for o in range(4):
        for dc in range(2):
            if o or dc:
                peers.append(dev_z(ring(zi, o), core ^ dc))
    for p in peers:
        pl.semaphore_signal(barrier, inc=1, device_id={"cp": p}, device_id_type=MESH)

    def rows_of(ref, h):
        return ref[:, :, h].astype(F32).reshape(HD, HD)

    for c in inputs[:2]:
        c.wait()
    for h in range(8):
        msg[h, :HD] = rows_of(in_q, h).astype(BF16)
        msg[h, HD:TK] = rows_of(in_do, h).astype(BF16)
    pl.semaphore_wait(barrier, len(peers))

    def got(ref, sem):
        rcopy(ref, ref, p_send.at[0], sem, me).wait_recv()

    def sent(ref, sem):
        rcopy(ref, ref, sem, l_r.at[0], me).wait_send()

    def to_head(a, dc):
        tc = core ^ dc
        tz = ring(zi, off(a, tc))
        tq, tk = jnp.where(tc == 0, xi, yi), jnp.where(tc == 0, yi, xi)
        return tz * 2 + tc, dev_z(tz, tc), tq, tk

    def q_msg(h):
        return msg.at[h, pl.ds(0, TK)].reshape(2, 2, QR, HD)

    def k_msg(h):
        return msg.at[h, pl.ds(TK, 2 * KR)].reshape(2, KR, HD)

    def a2a_q(a, dc):
        h, to, tq, _ = to_head(a, dc)
        rcopy(q_msg(h), qd.at[zi, :, :, tq, core], a_send.at[0], a_q.at[a, dc], to).start()

    def a2a_ld(a, dc):
        h, to, tq, _ = to_head(a, dc)
        rcopy(ld.at[h], ldg.at[zi, tq, core], a_send.at[2], a_l.at[a], to).start()

    def a2a_k(a, dc):
        h, to, _, tk = to_head(a, dc)
        rcopy(k_msg(h), kv.at[zi, :, tk, core], a_send.at[1], a_k.at[a, dc], to).start()

    def forward_q(a, dc):
        sz, sc = piece_z(a), core ^ dc
        c = qd.at[sz, :, :, gq, sc]
        if not (isinstance(a, int) and a == 0 and dc == 0):
            got(c, a_q.at[a, dc])
        for to in (dqo, dqp, dqm):
            rcopy(c, c, f_send.at[0], q_r.at[a], to).start()

    def forward_k(a, dc, wait=True):
        sz, sc = piece_z(a), core ^ dc
        c = kv.at[sz, :, gk, sc]
        if not (isinstance(a, int) and a == 0 and dc == 0) and wait:
            got(c, a_k.at[a, dc])
        for to in (dko, dkp, dkm):
            rcopy(c, c, f_send.at[1], k_r.at[a], to).start()

    def forward_ld(a):
        c = ldg.at[piece_z(a), gq]
        got(c.at[0] if isinstance(a, int) and a == 0 else c, a_l.at[a])
        for to in (dqp, dqm, dqo):
            rcopy(c, c, f_send.at[2], l_r.at[a], to).start()

    def arrive_q(a):
        sz = piece_z(a)
        got(qd.at[sz, :, :, 0:3], q_r.at[a])
        got(ldg.at[sz, 0:3], l_r.at[a])
        for b in range(2):
            qt[sz, b] = qd[sz, b].reshape(PQ, 128).T
        t = jnp.concatenate([ldg[sz].reshape(64, HD), jnp.zeros((64, HD), F32)], 0).T
        part_of = lax.broadcasted_iota(jnp.int32, (HD, HD), 1) >> 3
        t = jnp.concatenate([jnp.where(part_of == i, t, 0.0) for i in range(8)], 0).astype(BF16)
        r = jnp.dot(t, spread[...], preferred_element_type=F32)
        for i in range(8):
            x, rows = i // 2, pl.ds(i % 2 * 64, 64)
            for ref, v in ((lb, r[i * HD:(i + 1) * HD, :HD]), (db, r[i * HD:(i + 1) * HD, HD:])):
                ref[sz, 0, x, rows] = v[:64]
                ref[sz, 1, x, rows] = v[64:]

    def arrive_k(a):
        sz = piece_z(a)
        got(kv.at[sz, :, 0:3], k_r.at[a])
        for b in range(2):
            kt[sz, b] = kv[sz, b].reshape(PK, 128).T
        kn[sz] = kv[sz, 0].reshape(PK, 128)

    a2a_q(0, 1)
    for dc in (1, 0):
        for a in (1, 2):
            a2a_q(a, dc)
    qd[zi, :, :, gq, core] = msg[head, :TK].reshape(2, 2, QR, HD)
    forward_q(0, 0)
    for c, ref, r in ((inputs[2], in_k, TK), (inputs[3], in_v, TK + KR)):
        c.wait()
        rows32[...] = ref[...].astype(F32)
        for h in range(8):
            msg[h, r:r + KR] = rows32[:, h, :].astype(BF16)
    a2a_k(0, 1)
    for dc in (1, 0):
        for a in (1, 2):
            a2a_k(a, dc)
    kv[zi, :, gk, core] = msg[head, TK:].reshape(2, KR, HD)
    forward_k(0, 0)
    forward_q(0, 1)
    forward_k(0, 1)

    for c in inputs[4:]:
        c.wait()
    row = lax.broadcasted_iota(jnp.int32, (HD, HD), 0)
    lane = lax.broadcasted_iota(jnp.int32, (HD, HD), 1)
    lse = jnp.concatenate([in_lse[...].reshape(32, 32) * LOG2E, jnp.zeros((32, 96), F32)], 1)
    lse = jnp.broadcast_to(lse.reshape(32, 1, HD), (32, Z, HD)).reshape(HD, HD)
    def pieces(x):
        out = []
        for _ in range(3):
            out.append(x.astype(BF16).astype(F32))
            x = x - out[-1]
        return out

    for h in range(8):
        one = jnp.where(lane == Z * h + (row & 3), lse, 0.0)
        d = rows_of(in_do, h) * rows_of(in_o, h)
        ld[h] = jnp.concatenate([*pieces(jnp.sum(one.T, axis=0, keepdims=True)), *pieces(jnp.sum(d.T, axis=0, keepdims=True)),
                                 jnp.zeros((2, HD), F32)], 0)
    a2a_ld(0, 1)
    for dc in (1, 0):
        for a in (1, 2):
            a2a_ld(a, dc)
    ldg[zi, gq, core] = ld[head]
    forward_ld(0)
    kind = lax.broadcasted_iota(jnp.int32, (HD, 2 * HD), 0) & 7
    want = (lax.broadcasted_iota(jnp.int32, (HD, 2 * HD), 1) >> 7) * 3
    spread[...] = jnp.where(jnp.logical_and(kind >= want, kind < want + 3), 1.0, 0.0).astype(BF16)
    dq[...] = jnp.zeros_like(dq)
    acc[...] = jnp.zeros_like(acc)
    for dc in (1, 0):
        forward_q(1, dc)
    forward_ld(1)
    for f in (a2a_q, a2a_k, a2a_ld):
        for dc in (1, 0):
            f(3, dc)
    for dc in (1, 0):
        forward_q(2, dc)
    forward_ld(2)
    for dc in (1, 0):
        got(kv.at[piece_z(1), :, gk, core ^ dc], a_k.at[1, dc])
    arrive_q(0)
    arrive_k(0)
    for dc in (1, 0):
        forward_k(1, dc, wait=False)

    def block(zq, zk, ak, j, tiles, masked):
        if j is None:
            rows, rsl, jsl = PQ, slice(None), slice(None)
        else:
            rows, rsl, jsl = PQ // 2, pl.ds(pl.multiple_of(j * 512, 512), 512), j
        q = qd[zq, 0, jsl].reshape(rows, HD)
        do = qd[zq, 1, jsl].reshape(rows, HD)
        lrow = jnp.concatenate([lb[zq, jsl].reshape(rows, HD)] * 2, 1)
        drow = jnp.concatenate([db[zq, jsl].reshape(rows, HD)] * 2, 1)
        if masked:
            row = lax.broadcasted_iota(jnp.int32, (rows, HD), 0)
            qrow = jnp.concatenate([(row >> 2) + (row >> 7) * qstep] * 2, 1)
            qpos = prefix0 + zq * 512 + qbase + j * slice_len

        def products(k0):
            ks = pl.ds(k0, TK)
            return (jnp.dot(q, kt[zk, 0, :, ks], preferred_element_type=F32),
                    jnp.dot(do, kt[zk, 1, :, ks], preferred_element_type=F32))

        def weights(k0, s, dp):
            p = jnp.exp2(s * c2 - lrow)
            if masked:
                kid = lax.broadcasted_iota(jnp.int32, (1, TK), 1) + k0
                run = sum((kid >= i * 192).astype(jnp.int32) for i in range(1, Z))
                kpos = zk * 3072 + kbase + kid + run * kstep
                p = jnp.where(qrow >= kpos - qpos, p, 0.0)
            return p.astype(BF16), (p * (dp - drow)).astype(BF16)

        total = None
        ahead = products(tiles[0])
        for i, k0 in enumerate(tiles):
            pb, ds = weights(k0, *ahead)
            if i + 1 < len(tiles):
                ahead = products(tiles[i + 1])
            ks = pl.ds(k0, TK)
            acc[ak, 1, :, ks] += jnp.dot(qt[zq, 1, :, rsl], pb, preferred_element_type=F32)
            acc[ak, 0, :, ks] += jnp.dot(qt[zq, 0, :, rsl], ds, preferred_element_type=F32)
            r = jnp.dot(ds, kn[zk, ks], preferred_element_type=F32)
            total = r if total is None else total + r
        dq[zq, jsl] += total.reshape((2, Z, HD, HD) if j is None else (Z, HD, HD))

    ALL = (0, TK, 2 * TK)

    def cell(zq, zk, ak, j0=0, j1=2):
        base = zk * 3072 + kbase
        early = prefix0 + zq * 512 + qbase
        full = jnp.logical_and(base + 767 + 3 * kstep <= early, j1 - j0 == 2)

        @pl.when(full)
        def _():
            block(zq, zk, ak, None, ALL, False)

        @pl.when(jnp.logical_not(full))
        def _():
            def slice_j(j, _):
                q0 = early + j * slice_len
                last = q0 + 127 + 3 * qstep
                full_j = base + 767 + 3 * kstep <= q0
                seen2 = base + 512 + 2 * kstep <= last

                @pl.when(full_j)
                def _():
                    block(zq, zk, ak, j, ALL, False)

                @pl.when(jnp.logical_and(seen2, jnp.logical_not(full_j)))
                def _():
                    block(zq, zk, ak, j, ALL, True)

                @pl.when(jnp.logical_not(seen2))
                def _():
                    def tile_t(t, _):
                        @pl.when(base + t * (TK + kstep) <= last)
                        def _():
                            block(zq, zk, ak, j, (pl.multiple_of(t * TK, TK),), True)

                        return 0

                    lax.fori_loop(0, 2, tile_t, 0)

                return 0

            lax.fori_loop(j0, j1, slice_j, 0)

    h0, h1 = pl.ds(0, KR), pl.ds(KR, KR)

    def k_stepA(s):
        for b in range(2):
            t = acc[s, b].T
            if b == 0:
                t = t * inv_sqrt
            for y in range(4):
                part[s, y, b] = t[y * 2 * KR:(y + 1) * 2 * KR]
        rcopy(part.at[s, kO, :, h0], rak.at[s, 0], p_send.at[0], ka.at[s, 0], dkp).start()
        rcopy(part.at[s, kO, :, h1], rak.at[s, 1], p_send.at[0], ka.at[s, 1], dkm).start()
        rcopy(part.at[s, kP, :, h1], rbk.at[s, 0, :, h1], p_send.at[0], kb.at[s], dkp).start()
        rcopy(part.at[s, kM, :, h0], rbk.at[s, 1, :, h0], p_send.at[0], kb.at[s], dkm).start()

    def k_stepB(s):
        got(rak.at[s, 0], ka.at[s, 0])
        part[s, kP, :, :KR] = part[s, kP, :, :KR] + rak[s, 0]
        rcopy(part.at[s, kP, :, h0], rbk.at[s, 0, :, h0], p_send.at[0], kb.at[s], dkp).start()
        got(rak.at[s, 1], ka.at[s, 1])
        part[s, kM, :, KR:] = part[s, kM, :, KR:] + rak[s, 1]
        rcopy(part.at[s, kM, :, h1], rbk.at[s, 1, :, h1], p_send.at[0], kb.at[s], dkm).start()

    def k_stepC(s):
        got(rbk.at[s], kb.at[s])
        outk[s] = part[s, gk] + rbk[s, 0] + rbk[s, 1]
        tz = piece_z(s)

        def send(dc):
            tc = core ^ dc
            rows = pl.ds(pl.multiple_of(tc * 96, 96), 96)
            rcopy(outk.at[s, 0, rows], dk_out.at[head], o_send.at[0], o_r.at[0], dev_z(tz, tc)).start()
            rcopy(outk.at[s, 1, rows], dv_out.at[head], o_send.at[1], o_r.at[1], dev_z(tz, tc)).start()

        send(1)

        @pl.when(s > 0)
        def _():
            send(0)

        @pl.when(s == 0)
        def _():
            rows = pl.ds(pl.multiple_of(core * 96, 96), 96)
            dk_out[head] = outk[s, 0, rows]
            dv_out[head] = outk[s, 1, rows]

    def r_stepA(s):
        z = piece_z(s)
        rcopy(dq.at[z, 1, qO], raq.at[s, 1], p_send.at[1], qa.at[s, 1], dqm).start()
        rcopy(dq.at[z, 1, qP], rbq.at[s, 0, 1], p_send.at[1], qb.at[s], dqp).start()

    def q_stepA(s):
        z = piece_z(s)
        rcopy(dq.at[z, 0, qO], raq.at[s, 0], p_send.at[1], qa.at[s, 0], dqp).start()
        rcopy(dq.at[z, 0, qM], rbq.at[s, 1, 0], p_send.at[1], qb.at[s], dqm).start()
        pl.when(s > 0)(lambda: r_stepA(s))

    def r_stepB(s):
        z = piece_z(s)
        got(raq.at[s, 1], qa.at[s, 1])
        dq[z, 1, qM] = dq[z, 1, qM] + raq[s, 1]
        rcopy(dq.at[z, 1, qM], rbq.at[s, 1, 1], p_send.at[1], qb.at[s], dqm).start()

    def q_stepB(s):
        z = piece_z(s)
        got(raq.at[s, 0], qa.at[s, 0])
        dq[z, 0, qP] = dq[z, 0, qP] + raq[s, 0]
        rcopy(dq.at[z, 0, qP], rbq.at[s, 0, 0], p_send.at[1], qb.at[s], dqp).start()
        pl.when(s > 0)(lambda: r_stepB(s))

    def q_stepC(s):
        z = piece_z(s)
        got(rbq.at[s], qb.at[s])
        r = (dq[z, :, gq] + rbq[s, 0] + rbq[s, 1]) * inv_sqrt
        outq[s] = r.reshape(2, 2, 16, 4, HD).astype(BF16)

        def send(dc):
            tc = core ^ dc
            rcopy(outq.at[s, :, tc], dq_out.at[:, :, head], o_send.at[2], o_r.at[2], dev_z(z, tc)).start()

        send(1)

        @pl.when(s > 0)
        def _():
            send(0)

        @pl.when(s == 0)
        def _():
            dq_out[:, :, head] = outq[s, :, core]

    def word(digits, bits):
        v = sum(int(d) << (bits * i) for i, d in enumerate(digits))
        return jnp.int32(v - (1 << 32) if v >> 31 else v)

    def pick(table, n):
        return (word(table.replace(".", "0"), 2) >> (2 * n)) & 3

    def hit(tables, n):
        on = "".join("1" if any(t[i] != "." for t in tables) else "0" for i in range(16))
        return ((word(on, 1) >> n) & 1) == 1

    def at(table, n, f):
        @pl.when(hit([table], n))
        def _():
            f(pick(table, n))

    def both(f, last=None):
        def g(a):
            f(a, 1)
            f(a, 0)
            if last is not None:
                last(a)

        return g

    def group(parts, n):
        @pl.when(hit([t for t, _ in parts], n))
        def _():
            for t, f in parts:
                at(t, n, f)

    def step(n, _):
        group(((FORWARD_Q, both(forward_q, forward_ld)), (FORWARD_K, both(forward_k)),
               (ARRIVE_Q, arrive_q), (ARRIVE_K, arrive_k)), n)
        aq, ak = pick(QUERIES, n), pick(KEYS, n)
        cell(piece_z(aq), piece_z(ak), ak, jnp.where(n == 15, 1, 0))
        group(((KB, k_stepB), (QC, q_stepC), (QA, q_stepA), (RB, r_stepB), (KC, k_stepC), (QB, q_stepB), (RA, r_stepA), (KA, k_stepA)), n)
        return 0

    cell(zi, zi, 0, 0, 1)
    lax.fori_loop(0, 16, step, 0)
    steps = {"qB": q_stepB, "rB": r_stepB, "qC": q_stepC, "kB": k_stepB, "kC": k_stepC}
    for i in range(0, len(LAST), 3):
        steps[LAST[i:i + 2]](jnp.int32(int(LAST[i + 2])))

    got(dk_out.at[0:7], o_r.at[0])
    got(dv_out.at[0:7], o_r.at[1])
    got(dq_out.at[:, :, 0:7], o_r.at[2])
    sent(msg.at[0:7, pl.ds(0, TK)], a_send.at[0])
    sent(msg.at[0:7, pl.ds(TK, 2 * KR)], a_send.at[1])
    sent(ld.at[0:7], a_send.at[2])
    sent(qd.at[0:3], f_send.at[0])
    sent(kv.at[0:3], f_send.at[1])
    sent(ldg.at[0:3], f_send.at[2])
    sent(part.at[0:3], p_send.at[0])
    sent(dq.at[0:3], p_send.at[1])
    sent(dk_out.at[0:7], o_send.at[0])
    sent(dv_out.at[0:7], o_send.at[1])
    sent(dq_out.at[:, :, 0:7], o_send.at[2])


def store_kernel(dq, dk, dv, dq_out, dk_out, dv_out, dk_rows, dv_rows, sems):
    copies = [pltpu.make_async_copy(dq, dq_out, sems.at[0]), pltpu.make_async_copy(dk_rows, dk_out, sems.at[1]),
              pltpu.make_async_copy(dv_rows, dv_out, sems.at[2])]
    copies[0].start()
    for x, rows, c in ((dk, dk_rows, copies[1]), (dv, dv_rows, copies[2])):
        for h in range(8):
            rows[:, h, :] = x[h]
        c.start()
    for c in copies:
        c.wait()


def solution(mesh):
    cp_size = mesh.shape['cp']
    seq_spec = P(None, 'cp', 'heads', None)
    lse_spec = P(None, 'cp', 'heads')
    kv_spec = P('cp', 'heads', None)

    def local_backward(query, attn_out, grad_out, row_lse, key_cache, value_cache):
        n_slices, rows_dev, q_heads, head_dim = query.shape
        keys_dev, kv_heads, _ = key_cache.shape
        group = q_heads // kv_heads
        grp = (n_slices, rows_dev, kv_heads, group, head_dim)
        vm = pl.BlockSpec(memory_space=pltpu.VMEM)
        dma = pltpu.SemaphoreType.DMA
        shape = (n_slices, rows_dev, keys_dev, head_dim, cp_size)
        scratch = [
            pltpu.VMEM(grp, BF16),
            pltpu.VMEM(grp, BF16),
            pltpu.VMEM(grp, BF16),
            pltpu.VMEM(row_lse.shape, F32),
            pltpu.VMEM(key_cache.shape, BF16),
            pltpu.VMEM(key_cache.shape, BF16),
            pltpu.VMEM(key_cache.shape, F32),
            pltpu.VMEM((8, 448, HD), BF16),
            pltpu.VMEM((8, 8, HD), F32),
            dma((6,)),
            pltpu.VMEM((HD, 2 * HD), BF16),
            pltpu.VMEM((Z, 2, 2, Z, 2, 64, HD), BF16),
            pltpu.VMEM((Z, 2, Z, 2, KR, HD), BF16),
            pltpu.VMEM((Z, PK, HD), BF16),
            pltpu.VMEM((Z, Z, 2, 8, HD), F32),
            pltpu.VMEM((Z, 2, HD, PQ), BF16),
            pltpu.VMEM((Z, 2, HD, PK), BF16),
            pltpu.VMEM((Z, 2, Z, HD, HD), F32),
            pltpu.VMEM((Z, 2, Z, HD, HD), F32),
            pltpu.VMEM((Z, 2, Z, HD, HD), F32),
            pltpu.VMEM((Z, 2, HD, PK), F32),
            pltpu.VMEM((Z, Z, 2, 2 * KR, HD), F32),
            pltpu.VMEM((Z, 2, 2, KR, HD), F32),
            pltpu.VMEM((Z, 2, 2, 2 * KR, HD), F32),
            pltpu.VMEM((Z, 2, HD, HD), F32),
            pltpu.VMEM((Z, 2, 2, HD, HD), F32),
            pltpu.VMEM((Z, 2, 2 * KR, HD), F32),
            pltpu.VMEM((Z, 2, 2, 16, 4, HD), BF16),
            dma((3,)), dma((4, 2)), dma((4, 2)), dma((Z,)),
            dma((3,)), dma((Z,)), dma((Z,)), dma((Z,)),
            dma((4, 2)), dma((Z,)), dma((4, 2)), dma((Z,)),
            dma((2,)), dma((3,)), dma((3,)),
        ]
        dq, dk, dv = pl.pallas_call(
            functools.partial(kernel, shape),
            out_shape=[jax.ShapeDtypeStruct(grp, BF16), jax.ShapeDtypeStruct((8, KR, HD), F32),
                       jax.ShapeDtypeStruct((8, KR, HD), F32)],
            in_specs=[pl.BlockSpec(memory_space=pltpu.HBM)] * 6, out_specs=[vm] * 3, scratch_shapes=scratch,
            compiler_params=pltpu.CompilerParams(collective_id=0, has_side_effects=True, vmem_limit_bytes=46 * 2 ** 20),
            name="attn_bwd",
        )(*(pltpu.with_memory_space_constraint(a, pltpu.HBM) for a in (query.reshape(grp), attn_out.reshape(grp), grad_out.reshape(grp), row_lse, key_cache, value_cache)))
        hbm = pl.BlockSpec(memory_space=pl.ANY)
        dq, dk, dv = pl.pallas_call(
            store_kernel,
            out_shape=[jax.ShapeDtypeStruct(dq.shape, BF16), jax.ShapeDtypeStruct(key_cache.shape, F32),
                       jax.ShapeDtypeStruct(key_cache.shape, F32)],
            in_specs=[vm] * 3, out_specs=[hbm] * 3,
            scratch_shapes=[pltpu.VMEM(key_cache.shape, F32), pltpu.VMEM(key_cache.shape, F32), dma((3,))],
            compiler_params=pltpu.CompilerParams(vmem_limit_bytes=2 ** 22), name="store",
        )(dq, dk, dv)
        return dq.reshape(query.shape), dk, dv

    return jax.shard_map(local_backward, mesh=mesh, in_specs=(seq_spec, seq_spec, seq_spec, lse_spec, kv_spec, kv_spec),
                         out_specs=(seq_spec, kv_spec, kv_spec), check_vma=False)
```

```python
import functools

import jax
import jax.numpy as jnp
from jax import lax
from jax.experimental import pallas as pl
from jax.experimental.pallas import tpu as pltpu
from jax.sharding import PartitionSpec as P

F32 = jnp.float32
BF16 = jnp.bfloat16
MESH = pl.DeviceIdType.MESH
LOG2E = 1.4426950408889634
Z = 4
HD = 128
PQ = 1024
PK = 768
TK = 256
KR = 96
QR = 64


QUERIES = "1012301230123320"
KEYS = "0111133332222000"
FORWARD_Q = ".3.............."
FORWARD_K = "..3..2.........."
ARRIVE_Q = "1..23..........."
ARRIVE_K = ".1...3...2......"
KC = ".............1.3"
QC = "...............1"
KB = ".......1...3..2."
QB = "...........01..."
RB = "................"
QA = ".........01..32."
RA = "...............0"
KA = "....1...3...2..0"
LAST = "qB3qB2kC2qC3kB0rB0qC2kC0qC0"


def kernel(shape, query, attn_out, grad_out, row_lse, key_cache, value_cache, dq_out, dk_out, dv_out,
           in_q, in_o, in_do, in_lse, in_k, in_v, rows32, msg, ld, in_sems, spread, qd, kv, kn, ldg, qt, kt, lb, db,
           dq, acc, part, rak, rbk, raq, rbq, outk, outq,
           a_send, a_q, a_k, a_l, f_send, q_r, k_r, l_r,
           ka, kb, qa, qb, p_send, o_send, o_r):
    n_slices, rows_dev, keys_dev, head_dim, cp_size = shape
    slice_len = rows_dev * cp_size
    prefix0 = keys_dev * cp_size - n_slices * slice_len
    inv_sqrt = head_dim ** -0.5
    c2 = inv_sqrt * LOG2E
    me = lax.axis_index("cp")
    core = lax.rem(me, 2)
    xi = lax.rem(me // 2, 4)
    yi = lax.rem(me // 8, 4)
    zi = me // 32
    head = zi * 2 + core
    first = core == 0
    gq, gk = jnp.where(first, xi, yi), jnp.where(first, yi, xi)
    sq, sk = jnp.where(first, 2, 8), jnp.where(first, 8, 2)
    kbase, kstep = jnp.where(first, xi * 192, yi * PK), jnp.where(first, 576, 0)
    qbase, qstep = jnp.where(first, yi * 128, xi * 32), jnp.where(first, 0, 96)

    def ring(i, d):
        return lax.rem(i + d + 4, 4)

    qP, qM, qO = ring(gq, 1), ring(gq, -1), ring(gq, 2)
    kP, kM, kO = ring(gk, 1), ring(gk, -1), ring(gk, 2)
    dqp, dqm, dqo = me + (qP - gq) * sq, me + (qM - gq) * sq, me + (qO - gq) * sq
    dkp, dkm, dko = me + (kP - gk) * sk, me + (kM - gk) * sk, me + (kO - gk) * sk

    def dev_z(z, c):
        return z * 32 + yi * 8 + xi * 2 + c

    def off(a, c):
        o = a ^ (a >> 1)
        return jnp.where(c == 0, o, (Z - o) & 3)

    def piece_z(a):
        return ring(zi, -off(a, core))

    def rcopy(src, dst, ss, rs, to):
        return pltpu.make_async_remote_copy(src_ref=src, dst_ref=dst, send_sem=ss, recv_sem=rs,
                                            device_id={"cp": to}, device_id_type=MESH)

    inputs = [pltpu.make_async_copy(src, dst, in_sems.at[i]) for i, (src, dst) in enumerate((
        (query, in_q), (grad_out, in_do), (key_cache, in_k), (value_cache, in_v), (attn_out, in_o), (row_lse, in_lse)))]
    for c in inputs:
        c.start()

    barrier = pltpu.get_barrier_semaphore()
    peers = [dqp, dqm, dqo, dkp, dkm, dko]
    for o in range(4):
        for dc in range(2):
            if o or dc:
                peers.append(dev_z(ring(zi, o), core ^ dc))
    for p in peers:
        pl.semaphore_signal(barrier, inc=1, device_id={"cp": p}, device_id_type=MESH)

    def rows_of(ref, h):
        return ref[:, :, h].astype(F32).reshape(HD, HD)

    for c in inputs[:2]:
        c.wait()
    for h in range(8):
        msg[h, :HD] = rows_of(in_q, h).astype(BF16)
        msg[h, HD:TK] = rows_of(in_do, h).astype(BF16)
    pl.semaphore_wait(barrier, len(peers))

    def got(ref, sem):
        rcopy(ref, ref, p_send.at[0], sem, me).wait_recv()

    def sent(ref, sem):
        rcopy(ref, ref, sem, l_r.at[0], me).wait_send()

    def to_head(a, dc):
        tc = core ^ dc
        tz = ring(zi, off(a, tc))
        tq, tk = jnp.where(tc == 0, xi, yi), jnp.where(tc == 0, yi, xi)
        return tz * 2 + tc, dev_z(tz, tc), tq, tk

    def q_msg(h):
        return msg.at[h, pl.ds(0, TK)].reshape(2, 2, QR, HD)

    def k_msg(h):
        return msg.at[h, pl.ds(TK, 2 * KR)].reshape(2, KR, HD)

    def a2a_q(a, dc):
        h, to, tq, _ = to_head(a, dc)
        rcopy(q_msg(h), qd.at[zi, :, :, tq, core], a_send.at[0], a_q.at[a, dc], to).start()

    def a2a_ld(a, dc):
        h, to, tq, _ = to_head(a, dc)
        rcopy(ld.at[h], ldg.at[zi, tq, core], a_send.at[2], a_l.at[a], to).start()

    def a2a_k(a, dc):
        h, to, _, tk = to_head(a, dc)
        rcopy(k_msg(h), kv.at[zi, :, tk, core], a_send.at[1], a_k.at[a], to).start()

    def forward_q(a, dc):
        sz, sc = piece_z(a), core ^ dc
        c = qd.at[sz, :, :, gq, sc]
        if not (isinstance(a, int) and a == 0 and dc == 0):
            got(c, a_q.at[a, dc])
        for to in (dqo, dqp, dqm):
            rcopy(c, c, f_send.at[0], q_r.at[a], to).start()

    def forward_k(a, dc, wait=True):
        sz, sc = piece_z(a), core ^ dc
        c = kv.at[sz, :, gk, sc]
        if dc == 1 and wait:
            got(c if isinstance(a, int) else kv.at[sz, :, gk], a_k.at[a])
        for to in (dko, dkp, dkm):
            rcopy(c, c, f_send.at[1], k_r.at[a], to).start()

    def forward_ld(a):
        c = ldg.at[piece_z(a), gq]
        got(c.at[0] if isinstance(a, int) and a == 0 else c, a_l.at[a])
        for to in (dqp, dqm, dqo):
            rcopy(c, c, f_send.at[2], l_r.at[a], to).start()

    def arrive_q(a):
        sz = piece_z(a)
        got(qd.at[sz, :, :, 0:3], q_r.at[a])
        got(ldg.at[sz, 0:3], l_r.at[a])
        for b in range(2):
            qt[sz, b] = qd[sz, b].reshape(PQ, 128).T
        t = jnp.concatenate([ldg[sz].reshape(64, HD), jnp.zeros((64, HD), F32)], 0).T
        part_of = lax.broadcasted_iota(jnp.int32, (HD, HD), 1) >> 3
        t = jnp.concatenate([jnp.where(part_of == i, t, 0.0) for i in range(8)], 0).astype(BF16)
        r = jnp.dot(t, spread[...], preferred_element_type=F32)
        for i in range(8):
            x, rows = i // 2, pl.ds(i % 2 * 64, 64)
            for ref, v in ((lb, r[i * HD:(i + 1) * HD, :HD]), (db, r[i * HD:(i + 1) * HD, HD:])):
                ref[sz, 0, x, rows] = v[:64]
                ref[sz, 1, x, rows] = v[64:]

    def arrive_k(a):
        sz = piece_z(a)
        got(kv.at[sz, :, 0:3], k_r.at[a])
        for b in range(2):
            kt[sz, b] = kv[sz, b].reshape(PK, 128).T
        kn[sz] = kv[sz, 0].reshape(PK, 128)

    a2a_q(0, 1)
    for dc in (1, 0):
        for a in (1, 2):
            a2a_q(a, dc)
    qd[zi, :, :, gq, core] = msg[head, :TK].reshape(2, 2, QR, HD)
    forward_q(0, 0)
    for c, ref, r in ((inputs[2], in_k, TK), (inputs[3], in_v, TK + KR)):
        c.wait()
        rows32[...] = ref[...].astype(F32)
        for h in range(8):
            msg[h, r:r + KR] = rows32[:, h, :].astype(BF16)
    a2a_k(0, 1)
    for dc in (1, 0):
        for a in (1, 2):
            a2a_k(a, dc)
    kv[zi, :, gk, core] = msg[head, TK:].reshape(2, KR, HD)
    forward_k(0, 0)
    forward_q(0, 1)
    forward_k(0, 1)

    for c in inputs[4:]:
        c.wait()
    row = lax.broadcasted_iota(jnp.int32, (HD, HD), 0)
    lane = lax.broadcasted_iota(jnp.int32, (HD, HD), 1)
    lse = jnp.concatenate([in_lse[...].reshape(32, 32) * LOG2E, jnp.zeros((32, 96), F32)], 1)
    lse = jnp.broadcast_to(lse.reshape(32, 1, HD), (32, Z, HD)).reshape(HD, HD)
    def pieces(x):
        out = []
        for _ in range(3):
            out.append(x.astype(BF16).astype(F32))
            x = x - out[-1]
        return out

    for h in range(8):
        one = jnp.where(lane == Z * h + (row & 3), lse, 0.0)
        d = rows_of(in_do, h) * rows_of(in_o, h)
        ld[h] = jnp.concatenate([*pieces(jnp.sum(one.T, axis=0, keepdims=True)), *pieces(jnp.sum(d.T, axis=0, keepdims=True)),
                                 jnp.zeros((2, HD), F32)], 0)
    a2a_ld(0, 1)
    for dc in (1, 0):
        for a in (1, 2):
            a2a_ld(a, dc)
    ldg[zi, gq, core] = ld[head]
    forward_ld(0)
    kind = lax.broadcasted_iota(jnp.int32, (HD, 2 * HD), 0) & 7
    want = (lax.broadcasted_iota(jnp.int32, (HD, 2 * HD), 1) >> 7) * 3
    spread[...] = jnp.where(jnp.logical_and(kind >= want, kind < want + 3), 1.0, 0.0).astype(BF16)
    dq[...] = jnp.zeros_like(dq)
    acc[...] = jnp.zeros_like(acc)
    for dc in (1, 0):
        forward_q(1, dc)
    forward_ld(1)
    for f in (a2a_q, a2a_k, a2a_ld):
        for dc in (1, 0):
            f(3, dc)
    for dc in (1, 0):
        forward_q(2, dc)
    forward_ld(2)
    got(kv.at[piece_z(1), :, gk], a_k.at[1])
    arrive_q(0)
    arrive_k(0)
    for dc in (1, 0):
        forward_k(1, dc, wait=False)

    def block(zq, zk, ak, j, tiles, masked):
        if j is None:
            rows, rsl, jsl = PQ, slice(None), slice(None)
        else:
            rows, rsl, jsl = PQ // 2, pl.ds(pl.multiple_of(j * 512, 512), 512), j
        q = qd[zq, 0, jsl].reshape(rows, HD)
        do = qd[zq, 1, jsl].reshape(rows, HD)
        lrow = jnp.concatenate([lb[zq, jsl].reshape(rows, HD)] * 2, 1)
        drow = jnp.concatenate([db[zq, jsl].reshape(rows, HD)] * 2, 1)
        if masked:
            row = lax.broadcasted_iota(jnp.int32, (rows, HD), 0)
            qrow = jnp.concatenate([(row >> 2) + (row >> 7) * qstep] * 2, 1)
            qpos = prefix0 + zq * 512 + qbase + j * slice_len

        def products(k0):
            ks = pl.ds(k0, TK)
            return (jnp.dot(q, kt[zk, 0, :, ks], preferred_element_type=F32),
                    jnp.dot(do, kt[zk, 1, :, ks], preferred_element_type=F32))

        def weights(k0, s, dp):
            p = jnp.exp2(s * c2 - lrow)
            if masked:
                kid = lax.broadcasted_iota(jnp.int32, (1, TK), 1) + k0
                run = sum((kid >= i * 192).astype(jnp.int32) for i in range(1, Z))
                kpos = zk * 3072 + kbase + kid + run * kstep
                p = jnp.where(qrow >= kpos - qpos, p, 0.0)
            return p.astype(BF16), (p * (dp - drow)).astype(BF16)

        total = None
        ahead = products(tiles[0])
        for i, k0 in enumerate(tiles):
            pb, ds = weights(k0, *ahead)
            if i + 1 < len(tiles):
                ahead = products(tiles[i + 1])
            ks = pl.ds(k0, TK)
            acc[ak, 1, :, ks] += jnp.dot(qt[zq, 1, :, rsl], pb, preferred_element_type=F32)
            acc[ak, 0, :, ks] += jnp.dot(qt[zq, 0, :, rsl], ds, preferred_element_type=F32)
            r = jnp.dot(ds, kn[zk, ks], preferred_element_type=F32)
            total = r if total is None else total + r
        dq[zq, jsl] += total.reshape((2, Z, HD, HD) if j is None else (Z, HD, HD))

    ALL = (0, TK, 2 * TK)

    def cell(zq, zk, ak, j0=0, j1=2):
        base = zk * 3072 + kbase
        early = prefix0 + zq * 512 + qbase
        full = jnp.logical_and(base + 767 + 3 * kstep <= early, j1 - j0 == 2)

        @pl.when(full)
        def _():
            block(zq, zk, ak, None, ALL, False)

        @pl.when(jnp.logical_not(full))
        def _():
            def slice_j(j, _):
                q0 = early + j * slice_len
                last = q0 + 127 + 3 * qstep
                full_j = base + 767 + 3 * kstep <= q0
                seen2 = base + 512 + 2 * kstep <= last

                @pl.when(full_j)
                def _():
                    block(zq, zk, ak, j, ALL, False)

                @pl.when(jnp.logical_and(seen2, jnp.logical_not(full_j)))
                def _():
                    block(zq, zk, ak, j, ALL, True)

                @pl.when(jnp.logical_not(seen2))
                def _():
                    def tile_t(t, _):
                        @pl.when(base + t * (TK + kstep) <= last)
                        def _():
                            block(zq, zk, ak, j, (pl.multiple_of(t * TK, TK),), True)

                        return 0

                    lax.fori_loop(0, 2, tile_t, 0)

                return 0

            lax.fori_loop(j0, j1, slice_j, 0)

    h0, h1 = pl.ds(0, KR), pl.ds(KR, KR)

    def k_stepA(s):
        for b in range(2):
            t = acc[s, b].T
            if b == 0:
                t = t * inv_sqrt
            for y in range(4):
                part[s, y, b] = t[y * 2 * KR:(y + 1) * 2 * KR]
        rcopy(part.at[s, kO, :, h0], rak.at[s, 0], p_send.at[0], ka.at[s, 0], dkp).start()
        rcopy(part.at[s, kO, :, h1], rak.at[s, 1], p_send.at[0], ka.at[s, 1], dkm).start()
        rcopy(part.at[s, kP, :, h1], rbk.at[s, 0, :, h1], p_send.at[0], kb.at[s], dkp).start()
        rcopy(part.at[s, kM, :, h0], rbk.at[s, 1, :, h0], p_send.at[0], kb.at[s], dkm).start()

    def k_stepB(s):
        got(rak.at[s, 0], ka.at[s, 0])
        part[s, kP, :, :KR] = part[s, kP, :, :KR] + rak[s, 0]
        rcopy(part.at[s, kP, :, h0], rbk.at[s, 0, :, h0], p_send.at[0], kb.at[s], dkp).start()
        got(rak.at[s, 1], ka.at[s, 1])
        part[s, kM, :, KR:] = part[s, kM, :, KR:] + rak[s, 1]
        rcopy(part.at[s, kM, :, h1], rbk.at[s, 1, :, h1], p_send.at[0], kb.at[s], dkm).start()

    def k_stepC(s):
        got(rbk.at[s], kb.at[s])
        outk[s] = part[s, gk] + rbk[s, 0] + rbk[s, 1]
        tz = piece_z(s)

        def send(dc):
            tc = core ^ dc
            rows = pl.ds(pl.multiple_of(tc * 96, 96), 96)
            rcopy(outk.at[s, 0, rows], dk_out.at[head], o_send.at[0], o_r.at[0], dev_z(tz, tc)).start()
            rcopy(outk.at[s, 1, rows], dv_out.at[head], o_send.at[1], o_r.at[1], dev_z(tz, tc)).start()

        send(1)

        @pl.when(s > 0)
        def _():
            send(0)

        @pl.when(s == 0)
        def _():
            rows = pl.ds(pl.multiple_of(core * 96, 96), 96)
            dk_out[head] = outk[s, 0, rows]
            dv_out[head] = outk[s, 1, rows]

    def r_stepA(s):
        z = piece_z(s)
        rcopy(dq.at[z, 1, qO], raq.at[s, 1], p_send.at[1], qa.at[s, 1], dqm).start()
        rcopy(dq.at[z, 1, qP], rbq.at[s, 0, 1], p_send.at[1], qb.at[s], dqp).start()

    def q_stepA(s):
        z = piece_z(s)
        rcopy(dq.at[z, 0, qO], raq.at[s, 0], p_send.at[1], qa.at[s, 0], dqp).start()
        rcopy(dq.at[z, 0, qM], rbq.at[s, 1, 0], p_send.at[1], qb.at[s], dqm).start()
        pl.when(s > 0)(lambda: r_stepA(s))

    def r_stepB(s):
        z = piece_z(s)
        got(raq.at[s, 1], qa.at[s, 1])
        dq[z, 1, qM] = dq[z, 1, qM] + raq[s, 1]
        rcopy(dq.at[z, 1, qM], rbq.at[s, 1, 1], p_send.at[1], qb.at[s], dqm).start()

    def q_stepB(s):
        z = piece_z(s)
        got(raq.at[s, 0], qa.at[s, 0])
        dq[z, 0, qP] = dq[z, 0, qP] + raq[s, 0]
        rcopy(dq.at[z, 0, qP], rbq.at[s, 0, 0], p_send.at[1], qb.at[s], dqp).start()
        pl.when(s > 0)(lambda: r_stepB(s))

    def q_stepC(s):
        z = piece_z(s)
        got(rbq.at[s], qb.at[s])
        r = (dq[z, :, gq] + rbq[s, 0] + rbq[s, 1]) * inv_sqrt
        outq[s] = r.reshape(2, 2, 16, 4, HD).astype(BF16)

        def send(dc):
            tc = core ^ dc
            rcopy(outq.at[s, :, tc], dq_out.at[:, :, head], o_send.at[2], o_r.at[2], dev_z(z, tc)).start()

        send(1)

        @pl.when(s > 0)
        def _():
            send(0)

        @pl.when(s == 0)
        def _():
            dq_out[:, :, head] = outq[s, :, core]

    def word(digits, bits):
        v = sum(int(d) << (bits * i) for i, d in enumerate(digits))
        return jnp.int32(v - (1 << 32) if v >> 31 else v)

    def pick(table, n):
        return (word(table.replace(".", "0"), 2) >> (2 * n)) & 3

    def hit(tables, n):
        on = "".join("1" if any(t[i] != "." for t in tables) else "0" for i in range(16))
        return ((word(on, 1) >> n) & 1) == 1

    def at(table, n, f):
        @pl.when(hit([table], n))
        def _():
            f(pick(table, n))

    def both(f, last=None):
        def g(a):
            f(a, 1)
            f(a, 0)
            if last is not None:
                last(a)

        return g

    def group(parts, n):
        @pl.when(hit([t for t, _ in parts], n))
        def _():
            for t, f in parts:
                at(t, n, f)

    def step(n, _):
        group(((FORWARD_Q, both(forward_q, forward_ld)), (FORWARD_K, both(forward_k)),
               (ARRIVE_Q, arrive_q), (ARRIVE_K, arrive_k)), n)
        aq, ak = pick(QUERIES, n), pick(KEYS, n)
        cell(piece_z(aq), piece_z(ak), ak, jnp.where(n == 15, 1, 0))
        group(((KB, k_stepB), (QC, q_stepC), (QA, q_stepA), (RB, r_stepB), (KC, k_stepC), (QB, q_stepB), (RA, r_stepA), (KA, k_stepA)), n)
        return 0

    cell(zi, zi, 0, 0, 1)
    lax.fori_loop(0, 16, step, 0)
    steps = {"qB": q_stepB, "rB": r_stepB, "qC": q_stepC, "kB": k_stepB, "kC": k_stepC}
    for i in range(0, len(LAST), 3):
        steps[LAST[i:i + 2]](jnp.int32(int(LAST[i + 2])))

    got(dk_out.at[0:7], o_r.at[0])
    got(dv_out.at[0:7], o_r.at[1])
    got(dq_out.at[:, :, 0:7], o_r.at[2])
    sent(msg.at[0:7, pl.ds(0, TK)], a_send.at[0])
    sent(msg.at[0:7, pl.ds(TK, 2 * KR)], a_send.at[1])
    sent(ld.at[0:7], a_send.at[2])
    sent(qd.at[0:3], f_send.at[0])
    sent(kv.at[0:3], f_send.at[1])
    sent(ldg.at[0:3], f_send.at[2])
    sent(part.at[0:3], p_send.at[0])
    sent(dq.at[0:3], p_send.at[1])
    sent(dk_out.at[0:7], o_send.at[0])
    sent(dv_out.at[0:7], o_send.at[1])
    sent(dq_out.at[:, :, 0:7], o_send.at[2])


def store_kernel(dq, dk, dv, dq_out, dk_out, dv_out, dk_rows, dv_rows, sems):
    copies = [pltpu.make_async_copy(dq, dq_out, sems.at[0]), pltpu.make_async_copy(dk_rows, dk_out, sems.at[1]),
              pltpu.make_async_copy(dv_rows, dv_out, sems.at[2])]
    copies[0].start()
    for x, rows, c in ((dk, dk_rows, copies[1]), (dv, dv_rows, copies[2])):
        for h in range(8):
            rows[:, h, :] = x[h]
        c.start()
    for c in copies:
        c.wait()


def solution(mesh):
    cp_size = mesh.shape['cp']
    seq_spec = P(None, 'cp', 'heads', None)
    lse_spec = P(None, 'cp', 'heads')
    kv_spec = P('cp', 'heads', None)

    def local_backward(query, attn_out, grad_out, row_lse, key_cache, value_cache):
        n_slices, rows_dev, q_heads, head_dim = query.shape
        keys_dev, kv_heads, _ = key_cache.shape
        group = q_heads // kv_heads
        grp = (n_slices, rows_dev, kv_heads, group, head_dim)
        vm = pl.BlockSpec(memory_space=pltpu.VMEM)
        dma = pltpu.SemaphoreType.DMA
        shape = (n_slices, rows_dev, keys_dev, head_dim, cp_size)
        scratch = [
            pltpu.VMEM(grp, BF16),
            pltpu.VMEM(grp, BF16),
            pltpu.VMEM(grp, BF16),
            pltpu.VMEM(row_lse.shape, F32),
            pltpu.VMEM(key_cache.shape, BF16),
            pltpu.VMEM(key_cache.shape, BF16),
            pltpu.VMEM(key_cache.shape, F32),
            pltpu.VMEM((8, 448, HD), BF16),
            pltpu.VMEM((8, 8, HD), F32),
            dma((6,)),
            pltpu.VMEM((HD, 2 * HD), BF16),
            pltpu.VMEM((Z, 2, 2, Z, 2, 64, HD), BF16),
            pltpu.VMEM((Z, 2, Z, 2, KR, HD), BF16),
            pltpu.VMEM((Z, PK, HD), BF16),
            pltpu.VMEM((Z, Z, 2, 8, HD), F32),
            pltpu.VMEM((Z, 2, HD, PQ), BF16),
            pltpu.VMEM((Z, 2, HD, PK), BF16),
            pltpu.VMEM((Z, 2, Z, HD, HD), F32),
            pltpu.VMEM((Z, 2, Z, HD, HD), F32),
            pltpu.VMEM((Z, 2, Z, HD, HD), F32),
            pltpu.VMEM((Z, 2, HD, PK), F32),
            pltpu.VMEM((Z, Z, 2, 2 * KR, HD), F32),
            pltpu.VMEM((Z, 2, 2, KR, HD), F32),
            pltpu.VMEM((Z, 2, 2, 2 * KR, HD), F32),
            pltpu.VMEM((Z, 2, HD, HD), F32),
            pltpu.VMEM((Z, 2, 2, HD, HD), F32),
            pltpu.VMEM((Z, 2, 2 * KR, HD), F32),
            pltpu.VMEM((Z, 2, 2, 16, 4, HD), BF16),
            dma((3,)), dma((Z, 2)), dma((Z,)), dma((Z,)),
            dma((3,)), dma((Z,)), dma((Z,)), dma((Z,)),
            dma((Z, 2)), dma((Z,)), dma((Z, 2)), dma((Z,)),
            dma((2,)), dma((3,)), dma((3,)),
        ]
        dq, dk, dv = pl.pallas_call(
            functools.partial(kernel, shape),
            out_shape=[jax.ShapeDtypeStruct(grp, BF16), jax.ShapeDtypeStruct((8, KR, HD), F32),
                       jax.ShapeDtypeStruct((8, KR, HD), F32)],
            in_specs=[pl.BlockSpec(memory_space=pltpu.HBM)] * 6, out_specs=[vm] * 3, scratch_shapes=scratch,
            compiler_params=pltpu.CompilerParams(collective_id=0, has_side_effects=True, vmem_limit_bytes=46 * 2 ** 20),
            name="attn_bwd",
        )(*(pltpu.with_memory_space_constraint(a, pltpu.HBM) for a in (query.reshape(grp), attn_out.reshape(grp), grad_out.reshape(grp), row_lse, key_cache, value_cache)))
        hbm = pl.BlockSpec(memory_space=pl.ANY)
        dq, dk, dv = pl.pallas_call(
            store_kernel,
            out_shape=[jax.ShapeDtypeStruct(dq.shape, BF16), jax.ShapeDtypeStruct(key_cache.shape, F32),
                       jax.ShapeDtypeStruct(key_cache.shape, F32)],
            in_specs=[vm] * 3, out_specs=[hbm] * 3,
            scratch_shapes=[pltpu.VMEM(key_cache.shape, F32), pltpu.VMEM(key_cache.shape, F32), dma((3,))],
            compiler_params=pltpu.CompilerParams(vmem_limit_bytes=2 ** 22), name="store",
        )(dq, dk, dv)
        return dq.reshape(query.shape), dk, dv

    return jax.shard_map(local_backward, mesh=mesh, in_specs=(seq_spec, seq_spec, seq_spec, lse_spec, kv_spec, kv_spec),
                         out_specs=(seq_spec, kv_spec, kv_spec), check_vma=False)
```
